32 devices in a mesh: row: 4 (over z), col: 8 (over y, x, core).
Axes of the slice: x: 2, y: 2, z: 4, core: 2. Of those that a mesh axis runs over, the one named last changes fastest.
Arguments:
- grad_terms: bfloat16 [8, 2, 4096, 10240], P('col', None, 'row'), may hold values from -25 to 25, as said below
- row_moment: float32 [2, 4096], P(None, 'row'), may hold values from 0.01 to 3
- col_moment: float32 [2, 10240], P(None, 'col'), may hold values from 0.01 to 1
Outputs:
- update: float32 [2, 4096, 10240], P(None, 'row', 'col')
- new_rows: float32 [2, 4096], P(None, 'row')
- new_cols: float32 [2, 10240], P(None, 'col')
The draws below stay inside these ranges and needn't reach their ends.
Inputs may be any that keep to these rules, and one draw needn't show every extreme that they name: `grad_terms`: partial gradient terms of the 8 batch shards.
All inputs are finite; a program needn't handle non-finite values.
Results may differ from the reference program's by a relative error of at most 0.0003.
Values sent between devices are 32-bit elements; how exact they have to be, the bound alone decides.
A program may use at most 256 MiB of HBM per device.

```python
import math
import jax
import jax.numpy as jnp
from jax import lax

D = 4096
FF = 10240
MATS = 2
SOURCES = 8


def draw_grad_terms(key, part):
    subkeys = jax.random.split(key, 4)
    full_shape = (SOURCES, MATS, D, FF)
    chosen = jax.random.randint(subkeys[0], (), 0, MATS)
    factor = jnp.where(jnp.arange(MATS) == chosen, 1.0, 0.05).astype(jnp.float32)
    row_scale = jnp.exp(jax.random.uniform(subkeys[1], (MATS, D, 1), jnp.float32, jnp.log(0.3), jnp.log(3.0)))
    col_scale = jnp.exp(jax.random.uniform(subkeys[2], (MATS, 1, FF), jnp.float32, jnp.log(0.3), jnp.log(3.0)))
    base_values = 0.25 * jax.random.truncated_normal(subkeys[3], -4.0, 4.0, full_shape, jnp.float32)
    values = base_values * row_scale[None] * col_scale[None] * factor[None, :, None, None]
    return values.astype(jnp.bfloat16)


def draw_row_moment(key, part):
    subkeys = jax.random.split(jax.random.fold_in(key, 17), 1)
    position = jnp.arange(D, dtype=jnp.float32)[None, :] / jnp.float32(D - 1)
    rough = jnp.exp(jax.random.uniform(subkeys[0], (MATS, D), jnp.float32, jnp.log(0.02), jnp.log(0.2)))
    rising = jnp.exp(position * jnp.log(10.0))
    return (rough * rising).astype(jnp.float32)


def levels(rng, extent, pieces, smallest, top_value):
    def one(dim, shards_of):
        draws = jax.random.uniform(jax.random.fold_in(jax.random.fold_in(rng, 6), dim), (shards_of,), jnp.float32, smallest / len(pieces), top_value / len(pieces))
        return jnp.repeat(jnp.exp(draws), extent[dim] // shards_of).reshape((-1,) + (1,) * (len(extent) - dim - 1))

    gain = one(*pieces[0])
    for cut in pieces[1:]:
        gain = gain * one(*cut)
    return gain


def setup_inputs(seed: int = 0) -> dict:
    keys = jax.random.split(jax.random.key(seed), 4)
    grad_terms = draw_grad_terms(jax.random.fold_in(keys[3], 71), 0)
    row_moment = draw_row_moment(jax.random.fold_in(keys[3], 71), 0)
    col_moment = jnp.clip(jnp.exp(math.log(1.0) - 4.6051702 * jax.random.uniform(keys[2], (MATS, FF), jnp.float32) ** levels(keys[2], (MATS, FF), ((1, 8),), -0.2, 0.2)), 0.01, 1.0)
    return dict(grad_terms=grad_terms, row_moment=row_moment, col_moment=col_moment)


second_decay = 1.0 - 100.0 ** (-0.8)
tiny_square = 1e-30

def reference(grad_terms, row_moment, col_moment):

    def accumulate(source, running):
        return running + grad_terms[source].astype(jnp.float32)
    gradient = lax.fori_loop(0, grad_terms.shape[0], accumulate, jnp.zeros(grad_terms.shape[1:], jnp.float32))
    squares = gradient * gradient + tiny_square
    new_rows = second_decay * row_moment + (1.0 - second_decay) * lax.optimization_barrier(jnp.sum(squares, axis=2)) / FF
    new_cols = second_decay * col_moment + (1.0 - second_decay) * lax.optimization_barrier(jnp.sum(squares, axis=1)) / D
    row_level = lax.optimization_barrier(jnp.sum(new_rows, axis=1)) / D
    estimate = new_rows[:, :, None] * new_cols[:, None, :] / row_level[:, None, None]
    raw_update = gradient / jnp.sqrt(estimate)
    clip_scale = jnp.maximum(1.0, jnp.sqrt(lax.optimization_barrier(jnp.sum(raw_update * raw_update, axis=(1, 2))) / (D * FF)))
    update = raw_update / clip_scale[:, None, None]
    return (update, new_rows, new_cols)
```

```python
import functools

import jax
import jax.numpy as jnp
from jax import lax
from jax.experimental import pallas as pl
from jax.experimental.pallas import tpu as pltpu
from jax.sharding import PartitionSpec as P

MESH = pl.DeviceIdType.MESH
second_decay = 1.0 - 100.0 ** (-0.8)
tiny_square = 1e-30
LANES = 128
PIECE = 64
CHUNK = 16


def flip(me, r):
    bit = 1
    while bit <= r:
        if r & bit:
            me = me + bit * (1 - 2 * lax.rem(me // bit, 2))
        bit *= 2
    return me


class Plan:
    def __init__(self, n, nz, mats, rows, width):
        bits = [1 << b for b in range(n.bit_length() - 1)]
        self.n, self.nz, self.mats, self.rows, self.width = n, nz, mats, rows, width
        self.orders = (bits, bits[:1] + bits[:0:-1])
        self.stages = len(bits) - 1
        self.first = [r for r in range(n) if not r & bits[0]]
        self.first_bit = bits[0]
        self.kept = []
        self.sent = []
        held = [list(self.first), list(self.first)]
        for s in range(1, self.stages + 1):
            sent = [[r for r in held[h] if r & self.orders[h][s]] for h in (0, 1)]
            held = [[r for r in held[h] if not r & self.orders[h][s]] for h in (0, 1)]
            self.sent.append(sent)
            self.kept.append([list(x) for x in held])
        self.piece = PIECE
        self.pieces = mats * rows // self.piece
        self.blocks = mats * rows // LANES
        L = self.stages
        self.offset = [2 * (L - 1) + 1] + [2 * (L - s) for s in range(1, L + 1)]
        self.acc_slots = self.offset[0] + 4
        self.send_slots = 3
        self.load_slots = 4
        self.recv_slots = [6] * (L - 1) + [4]


def kernel(plan, ff, d, grad_terms, row_moment, col_moment, gradient, row_gain, col_gain, new_rows, new_cols, *scratch):
    n, nz, mats, rows, width = plan.n, plan.nz, plan.mats, plan.rows, plan.width
    L, R, half = plan.stages, plan.piece, plan.piece // 2
    total = mats * rows
    (loaded, to_send, acc, grad, row_part, row_mine, row_all, nr_all, nr_sum, col_sum, w_sum, col_all, nc_all, sq_all,
     load_sem, first_send, first_recv, out_sem, row_send, row_recv, col_send, col_recv, sq_send, sq_recv, *rest) = scratch
    recv, send_sem, recv_sem = rest[:L], rest[L:2 * L], rest[2 * L:3 * L]
    me, my_row = lax.axis_index("col"), lax.axis_index("row")
    everyone = n * nz
    mine = my_row * n + me

    def other(i):
        q = lax.rem(mine + i, everyone)
        return q, {"row": q // n, "col": lax.rem(q, n)}

    def remote(src, dst, send, rcv, target):
        return pltpu.make_async_remote_copy(
            src_ref=src, dst_ref=dst, send_sem=send, recv_sem=rcv, device_id=target, device_id_type=MESH
        )

    def col_device(c):
        return {"row": my_row, "col": c}

    sibling = col_device(flip(me, plan.first_bit))

    def loads(p):
        slot = lax.rem(p, plan.load_slots)
        at = pl.multiple_of(p * R, R)
        out = []
        for r in range(n):
            c = pl.multiple_of(flip(me, r) * width, LANES)
            out.append(
                pltpu.make_async_copy(
                    grad_terms.at[pl.ds(at, R), pl.ds(c, width)], loaded.at[slot, r], load_sem.at[slot, r]
                )
            )
        return out

    def first_copy(p):
        return remote(
            to_send.at[lax.rem(p, plan.send_slots)],
            acc.at[lax.rem(p, plan.acc_slots)],
            first_send.at[lax.rem(p, plan.send_slots)],
            first_recv.at[lax.rem(p, plan.acc_slots)],
            sibling,
        )

    def stage_copies(s, h, p):
        slot = lax.rem(p, plan.recv_slots[s - 1])
        bit = plan.orders[h][s]
        target = col_device(flip(me, bit))
        out = []
        for r in plan.sent[s - 1][h]:
            j = plan.kept[s - 1][h].index(r ^ bit)
            out.append(
                remote(
                    acc.at[lax.rem(p, plan.acc_slots), plan.first.index(r), pl.ds(h * half, half)],
                    recv[s - 1].at[slot, h, j],
                    send_sem[s - 1].at[slot, h, j],
                    recv_sem[s - 1].at[slot, h, j],
                    target,
                )
            )
        return out

    def out_copy(p):
        at = pl.multiple_of(p * R, R)
        return pltpu.make_async_copy(grad.at[pl.ds(at, R)], gradient.at[pl.ds(at, R)], out_sem.at[lax.rem(p, 4)])

    def row_copies(k):
        return [
            remote(row_all.at[k, me], row_all.at[k, me], row_send.at[k, i - 1], row_recv.at[k, me], col_device(flip(me, i)))
            for i in range(1, n)
        ]

    def row_arrivals(k):
        for i in range(1, n):
            c = flip(me, i)
            yield remote(row_all.at[k, c], row_all.at[k, c], row_send.at[k, i - 1], row_recv.at[k, c], col_device(c))

    def z_peer(i):
        return lax.rem(my_row + i, nz)

    def col_copy(m, i):
        return remote(
            col_all.at[m, my_row], col_all.at[m, my_row], col_send.at[m, i - 1], col_recv.at[m, my_row],
            {"row": z_peer(i), "col": me},
        )

    def col_arrival(m, i):
        z = z_peer(i)
        return remote(
            col_all.at[m, z], col_all.at[m, z], col_send.at[m, i - 1], col_recv.at[m, z], {"row": z, "col": me}
        )

    def sq_copy(m, i):
        q, target = other(i)
        return remote(sq_all.at[m, mine], sq_all.at[m, mine], sq_send.at[m, i - 1], sq_recv.at[m, mine], target)

    def sq_arrival(m, i):
        q, target = other(i)
        return remote(sq_all.at[m, q], sq_all.at[m, q], sq_send.at[m, i - 1], sq_recv.at[m, q], target)

    def load_step(p):
        for c in loads(p):
            c.start()

    def send_step(p):
        slot, into = lax.rem(p, plan.load_slots), lax.rem(p, plan.send_slots)

        @pl.when(p >= plan.send_slots)
        def _():
            first_copy(p - plan.send_slots).wait_send()

        for c in loads(p):
            c.wait()

        @pl.loop(0, R // CHUNK)
        def _(i):
            at = pl.ds(pl.multiple_of(i * CHUNK, CHUNK), CHUNK)
            for j, r in enumerate(plan.first):
                to_send[into, j, at] = loaded[slot, r ^ plan.first_bit, at].astype(jnp.float32)

        first_copy(p).start()

    def add_own(p, h, r):
        slot, a = lax.rem(p, plan.load_slots), lax.rem(p, plan.acc_slots)
        j = plan.first.index(r)

        @pl.loop(0, half // CHUNK)
        def _(i):
            at = pl.ds(pl.multiple_of(h * half + i * CHUNK, CHUNK), CHUNK)
            acc[a, j, at] += loaded[slot, r, at].astype(jnp.float32)

    def stage_one(p):
        first_copy(p).wait_recv()
        for group in (plan.sent[0], plan.kept[0]):
            for h in (0, 1):
                for r in group[h]:
                    add_own(p, h, r)
        for s0, s1 in zip(stage_copies(1, 0, p), stage_copies(1, 1, p)):
            s0.start()
            s1.start()

    def add_received(s, h, p):
        slot, a = lax.rem(p, plan.recv_slots[s - 1]), lax.rem(p, plan.acc_slots)
        for k, r in enumerate(plan.kept[s - 1][h]):
            j = plan.first.index(r)

            @pl.loop(0, half // CHUNK)
            def _(i):
                inside = pl.multiple_of(i * CHUNK, CHUNK)
                at = pl.ds(h * half + inside, CHUNK)
                acc[a, j, at] += recv[s - 1][slot, h, k, pl.ds(inside, CHUNK)]

    def stage_later(s, p):
        for h in (0, 1):
            for c in stage_copies(s - 1, h, p):
                c.wait()
            add_received(s - 1, h, p)
        for h in (0, 1):
            for c in stage_copies(s, h, p):
                c.start()

    def matrix_of(p):
        return (p * R) // rows

    def final_step(p):
        slot, a, m = lax.rem(p, plan.recv_slots[L - 1]), lax.rem(p, plan.acc_slots), matrix_of(p)
        for h in (0, 1):
            for c in stage_copies(L, h, p):
                c.wait()

            @pl.loop(0, half // CHUNK)
            def _(i):
                inside = pl.multiple_of(i * CHUNK, CHUNK)
                at = h * half + inside
                g = acc[a, 0, pl.ds(at, CHUNK)] + recv[L - 1][slot, h, 0, pl.ds(inside, CHUNK)]
                grad[pl.ds(p * R + at, CHUNK)] = g
                q = g * g + tiny_square
                lane = q[:, :LANES]
                for j in range(1, width // LANES):
                    lane = lane + q[:, j * LANES:(j + 1) * LANES]
                row_part[pl.ds(pl.multiple_of(lax.rem(p * R, LANES) + at, CHUNK), CHUNK)] = lane
                col_sum[m] += sum(q[8 * j:8 * j + 8] for j in range(CHUNK // 8))

        @pl.when(p >= 4)
        def _():
            out_copy(p - 4).wait()

        out_copy(p).start()

        @pl.when(lax.rem((p + 1) * R, rows) == 0)
        def _():
            col_all[m, my_row] = jnp.sum(col_sum[m], axis=0, keepdims=True)

        @pl.when(lax.rem((p + 1) * R, LANES) == 0)
        def _():
            k = (p * R) // LANES
            row_all[k, me] = jnp.sum(row_part[...].T, axis=0, keepdims=True)
            for c in row_copies(k):
                c.start()

        @pl.when(lax.rem((p + 1) * R, rows) == 0)
        def _():
            for i in range(1, nz):
                col_copy(m, i).start()

    def block_step(k):
        m = (k * LANES) // rows
        for c in row_arrivals(k):
            c.wait_recv()
        full = row_all[k, 0]
        for c in range(1, n):
            full = full + row_all[k, c]
        fresh = second_decay * row_mine[k] + (1.0 - second_decay) * full / ff
        nr_all[k] = fresh
        nr_sum[m] += fresh
        inverse = jnp.broadcast_to(1.0 / fresh, (LANES, LANES)).T
        row_part_inv = inverse

        for i in range(LANES // 8):
            g = grad[pl.ds(pl.multiple_of(k * LANES + 8 * i, 8), 8)]
            q = g * g
            w = row_part_inv[8 * i:8 * i + 8]
            w_sum[m] += jnp.concatenate([q[:, j * LANES:(j + 1) * LANES] * w for j in range(width // LANES)], axis=1)

        for c in row_copies(k):
            c.wait_send()

    def matrix_step(m):
        for i in range(1, nz):
            col_arrival(m, i).wait_recv()
        full = col_all[m, 0]
        for z in range(1, nz):
            full = full + col_all[m, z]
        fresh = second_decay * col_moment_of(m) + (1.0 - second_decay) * full / d
        nc_all[m] = fresh
        w = jnp.sum(w_sum[m], axis=0, keepdims=True) / fresh
        part = w[:, :LANES]
        for j in range(1, width // LANES):
            part = part + w[:, j * LANES:(j + 1) * LANES]
        sq_all[m, mine] = jnp.concatenate([part, nr_sum[m]], axis=1)

        @pl.loop(1, everyone)
        def _(i):
            sq_copy(m, i).start()

        for i in range(1, nz):
            col_copy(m, i).wait_send()

    def col_moment_of(m):
        return nc_all[m]

    def scale_step(m):
        @pl.loop(1, everyone)
        def _(i):
            sq_arrival(m, i).wait_recv()

        both = jnp.sum(sq_all[m], axis=0)
        square = jnp.sum(both[:, :LANES], axis=1, keepdims=True)
        level = jnp.sum(both[:, LANES:], axis=1, keepdims=True) / (n * d)
        clip = jnp.maximum(1.0, jnp.sqrt(square * level / (d * ff)))
        col_gain[pl.ds(m, 1), :] = lax.rsqrt(nc_all[m]) * (jnp.sqrt(level) / clip)
        new_cols[pl.ds(m, 1), :] = nc_all[m]

        @pl.loop(1, everyone)
        def _(i):
            sq_copy(m, i).wait_send()

    o = plan.offset
    for p in range(3):
        load_step(p)
    barrier = pltpu.get_barrier_semaphore()

    @pl.loop(1, everyone)
    def _(i):
        q, target = other(i)
        pl.semaphore_signal(barrier, inc=1, device_id=target, device_id_type=MESH)

    for m in range(mats):
        nc_all[m] = col_moment[m:m + 1, :]
        for k in range(rows // LANES):
            row_mine[m * (rows // LANES) + k] = row_moment[m:m + 1, k * LANES:(k + 1) * LANES]
    nr_sum[...] = jnp.zeros_like(nr_sum)
    col_sum[...] = jnp.zeros_like(col_sum)
    w_sum[...] = jnp.zeros_like(w_sum)
    pl.semaphore_wait(barrier, everyone - 1)

    per_block = LANES // R
    late = 2

    @pl.loop(-o[0], plan.pieces + 1)
    def _(t):
        def run(p, step):
            pl.when(jnp.logical_and(p >= 0, p < plan.pieces))(lambda: step(p))

        run(t + o[1], stage_one)
        for s in range(2, L + 1):
            run(t + o[s], functools.partial(stage_later, s))
        run(t - 1, final_step)
        run(t + o[0], send_step)
        pl.when(jnp.logical_and(t + o[0] + 3 < plan.pieces, t + o[0] >= 0))(lambda: load_step(t + o[0] + 3))
        done = t - 1 - late

        @pl.when(jnp.logical_and(done >= 0, lax.rem(done + 1, per_block) == 0))
        def _():
            k = done // per_block
            block_step(k)
            pl.when(lax.rem((k + 1) * LANES, rows) == 0)(lambda: matrix_step((k * LANES) // rows))

    seen = plan.pieces - 1 - late
    for k in range((seen + 1) // per_block, plan.blocks):
        block_step(k)
        if (k + 1) * LANES % rows == 0:
            matrix_step(k * LANES // rows)
    for m in range(mats):
        for k in range(rows // LANES):
            b = m * (rows // LANES) + k
            new_rows[m:m + 1, k * LANES:(k + 1) * LANES] = nr_all[b]
            row_gain[m:m + 1, k * LANES:(k + 1) * LANES] = lax.rsqrt(nr_all[b])
    for m in range(mats):
        scale_step(m)
    for p in range(plan.pieces - plan.send_slots, plan.pieces):
        first_copy(p).wait_send()
    for p in range(plan.pieces - 4, plan.pieces):
        out_copy(p).wait()


def on_device(n, nz, grad_terms, row_moment, col_moment):
    mats, rows, ff = grad_terms.shape[1:]
    width = ff // n
    d = rows * nz
    plan = Plan(n, nz, mats, rows, width)
    L, R, half, everyone = plan.stages, plan.piece, plan.piece // 2, n * nz
    kept = [len(plan.kept[s][0]) for s in range(L)]
    f32 = jnp.float32
    dma = pltpu.SemaphoreType.DMA
    blocks = plan.blocks
    scratch = [
        pltpu.VMEM((plan.load_slots, n, R, width), grad_terms.dtype),
        pltpu.VMEM((plan.send_slots, n // 2, R, width), f32),
        pltpu.VMEM((plan.acc_slots, n // 2, R, width), f32),
        pltpu.VMEM((mats * rows, width), f32),
        pltpu.VMEM((LANES, LANES), f32),
        pltpu.VMEM((blocks, 1, LANES), f32),
        pltpu.VMEM((blocks, n, 1, LANES), f32),
        pltpu.VMEM((blocks, 1, LANES), f32),
        pltpu.VMEM((mats, 1, LANES), f32),
        pltpu.VMEM((mats, 8, width), f32),
        pltpu.VMEM((mats, 8, width), f32),
        pltpu.VMEM((mats, nz, 1, width), f32),
        pltpu.VMEM((mats, 1, width), f32),
        pltpu.VMEM((mats, everyone, 1, 2 * LANES), f32),
        dma((plan.load_slots, n)),
        dma((plan.send_slots,)),
        dma((plan.acc_slots,)),
        dma((4,)),
        dma((blocks, n - 1)),
        dma((blocks, n)),
        dma((mats, nz - 1)),
        dma((mats, nz)),
        dma((mats, everyone - 1)),
        dma((mats, everyone)),
    ]
    scratch += [pltpu.VMEM((plan.recv_slots[s], 2, kept[s], half, width), f32) for s in range(L)]
    scratch += [dma((plan.recv_slots[s], 2, kept[s])) for s in range(L)] * 2
    vmem, anywhere = pl.BlockSpec(memory_space=pltpu.VMEM), pl.BlockSpec(memory_space=pl.ANY)
    gradient, row_gain, col_gain, new_rows, new_cols = pl.pallas_call(
        functools.partial(kernel, plan, ff, d),
        out_shape=(
            jax.ShapeDtypeStruct((mats * rows, width), f32),
            jax.ShapeDtypeStruct((mats, rows), f32),
            jax.ShapeDtypeStruct((mats, width), f32),
            jax.ShapeDtypeStruct((mats, rows), f32),
            jax.ShapeDtypeStruct((mats, width), f32),
        ),
        in_specs=[anywhere, vmem, vmem],
        out_specs=(anywhere, vmem, vmem, vmem, vmem),
        scratch_shapes=scratch,
        compiler_params=pltpu.CompilerParams(
            collective_id=0, has_side_effects=True, vmem_limit_bytes=56 * 1024 * 1024
        ),
        name="reduce_and_level",
    )(grad_terms.reshape(mats * rows, ff), row_moment, col_moment)
    gradient = gradient.reshape(mats, rows, width)
    update = gradient * row_gain[:, :, None] * col_gain[:, None, :]
    return update, new_rows, new_cols


def solution(mesh):
    n, nz = mesh.shape["col"], mesh.shape["row"]
    return jax.shard_map(
        functools.partial(on_device, n, nz),
        mesh=mesh,
        in_specs=(P("col", None, "row", None), P(None, "row"), P(None, "col")),
        out_specs=(P(None, "row", "col"), P(None, "row"), P(None, "col")),
        check_vma=False,
    )
```

```python
import functools

import jax
import jax.numpy as jnp
from jax import lax
from jax.experimental import pallas as pl
from jax.experimental.pallas import tpu as pltpu
from jax.sharding import PartitionSpec as P

MESH = pl.DeviceIdType.MESH
second_decay = 1.0 - 100.0 ** (-0.8)
tiny_square = 1e-30
LANES = 128
PIECE = 64
CHUNK = 16


def flip(me, r):
    bit = 1
    while bit <= r:
        if r & bit:
            me = me + bit * (1 - 2 * lax.rem(me // bit, 2))
        bit *= 2
    return me


class Plan:
    def __init__(self, n, nz, mats, rows, width):
        bits = [1 << b for b in range(n.bit_length() - 1)]
        self.n, self.nz, self.mats, self.rows, self.width = n, nz, mats, rows, width
        self.orders = (bits, bits[:1] + bits[:0:-1])
        self.stages = len(bits) - 1
        self.first = [r for r in range(n) if not r & bits[0]]
        self.first_bit = bits[0]
        self.kept = []
        self.sent = []
        held = [list(self.first), list(self.first)]
        for s in range(1, self.stages + 1):
            sent = [[r for r in held[h] if r & self.orders[h][s]] for h in (0, 1)]
            held = [[r for r in held[h] if not r & self.orders[h][s]] for h in (0, 1)]
            self.sent.append(sent)
            self.kept.append([list(x) for x in held])
        self.piece = PIECE
        self.pieces = mats * rows // self.piece
        self.blocks = mats * rows // LANES
        L = self.stages
        self.offset = [2 * (L - 1) + 1] + [2 * (L - s) for s in range(1, L + 1)]
        self.acc_slots = self.offset[0] + 4
        self.send_slots = 3
        self.load_slots = 4
        self.recv_slots = [6] * (L - 1) + [4]


def kernel(plan, ff, d, grad_terms, row_moment, col_moment, grad, col_gain, new_rows, new_cols, *scratch):
    n, nz, mats, rows, width = plan.n, plan.nz, plan.mats, plan.rows, plan.width
    L, R, half = plan.stages, plan.piece, plan.piece // 2
    (loaded, to_send, acc, row_old, col_old, row_part, row_mine, row_all, nr_sum, col_sum, w_sum, col_all, sq_all,
     load_sem, first_send, first_recv, old_sem, row_send, row_recv, col_send, col_recv, sq_send, sq_recv, *rest) = scratch
    recv, send_sem, recv_sem = rest[:L], rest[L:2 * L], rest[2 * L:3 * L]
    me, my_row = lax.axis_index("col"), lax.axis_index("row")
    peer = [flip(me, r) for r in range(n)]
    level = [lax.rem(my_row + i, nz) for i in range(nz)]
    far = [(i, r) for i in range(nz - 1, -1, -1) for r in range(n - 1, -1, -1) if i or r]

    def remote(src, dst, send, rcv, i, r):
        return pltpu.make_async_remote_copy(
            src_ref=src, dst_ref=dst, send_sem=send, recv_sem=rcv,
            device_id={"row": level[i], "col": peer[r]}, device_id_type=MESH,
        )

    def load(p, r):
        slot = lax.rem(p, plan.load_slots)
        at = pl.multiple_of(p * R, R)
        c = pl.multiple_of(peer[r] * width, LANES)
        return pltpu.make_async_copy(
            grad_terms.at[pl.ds(at, R), pl.ds(c, width)], loaded.at[slot, r], load_sem.at[slot, r]
        )

    def first_copy(p, j):
        a, b = lax.rem(p, plan.send_slots), lax.rem(p, plan.acc_slots)
        return remote(to_send.at[a, j], acc.at[b, j], first_send.at[a, j], first_recv.at[b, j], 0, plan.first_bit)

    def stage_copy(s, h, p, r):
        slot = lax.rem(p, plan.recv_slots[s - 1])
        bit = plan.orders[h][s]
        j = plan.kept[s - 1][h].index(r ^ bit)
        return remote(
            acc.at[lax.rem(p, plan.acc_slots), plan.first.index(r), pl.ds(h * half, half)],
            recv[s - 1].at[slot, h, j],
            send_sem[s - 1].at[slot, h, j],
            recv_sem[s - 1].at[slot, h, j],
            0,
            bit,
        )

    def stage_copies(s, h, p):
        return [stage_copy(s, h, p, r) for r in plan.sent[s - 1][h]]

    def row_copy(k, r):
        return remote(row_all.at[k, me], row_all.at[k, me], row_send.at[k, r - 1], row_recv.at[k, me], 0, r)

    def row_arrival(k, r):
        c = peer[r]
        return remote(row_all.at[k, c], row_all.at[k, c], row_send.at[k, r - 1], row_recv.at[k, c], 0, r)

    def col_copy(m, i):
        return remote(col_all.at[m, my_row], col_all.at[m, my_row], col_send.at[m, i - 1], col_recv.at[m, my_row], i, 0)

    def col_arrival(m, i):
        z = level[i]
        return remote(col_all.at[m, z], col_all.at[m, z], col_send.at[m, i - 1], col_recv.at[m, z], i, 0)

    def sq_copy(m, i, r):
        here = sq_all.at[m, my_row, me]
        return remote(here, here, sq_send.at[m, i, r], sq_recv.at[m, my_row, me], i, r)

    def sq_arrival(m, i, r):
        there = sq_all.at[m, level[i], peer[r]]
        return remote(there, there, sq_send.at[m, i, r], sq_recv.at[m, level[i], peer[r]], i, r)

    def load_step(p):
        for r in plan.first:
            load(p, r ^ plan.first_bit).start()
        for r in plan.first:
            load(p, r).start()

    def send_step(p):
        slot, into = lax.rem(p, plan.load_slots), lax.rem(p, plan.send_slots)
        waiting = None
        for j, r in enumerate(plan.first):
            pl.when(p >= plan.send_slots)(lambda: first_copy(p - plan.send_slots, j).wait_send())
            load(p, r ^ plan.first_bit).wait()

            @pl.loop(0, R // CHUNK)
            def _(i):
                at = pl.ds(pl.multiple_of(i * CHUNK, CHUNK), CHUNK)
                to_send[into, j, at] = loaded[slot, r ^ plan.first_bit, at].astype(jnp.float32)

            if waiting is not None:
                waiting.start()
            waiting = first_copy(p, j)
        waiting.start()

    def stage_one(p):
        slot, a = lax.rem(p, plan.load_slots), lax.rem(p, plan.acc_slots)
        waiting = []
        for j, r in enumerate(plan.first):
            load(p, r).wait()
            first_copy(p, j).wait_recv()

            @pl.loop(0, R // CHUNK)
            def _(i):
                at = pl.ds(pl.multiple_of(i * CHUNK, CHUNK), CHUNK)
                acc[a, j, at] += loaded[slot, r, at].astype(jnp.float32)

            for c in waiting:
                c.start()
            waiting = [stage_copy(1, h, p, r) for h in (0, 1) if r in plan.sent[0][h]]
        for c in waiting:
            c.start()

    def add_received(s, h, p):
        slot, a = lax.rem(p, plan.recv_slots[s - 1]), lax.rem(p, plan.acc_slots)
        for k, r in enumerate(plan.kept[s - 1][h]):
            j = plan.first.index(r)

            @pl.loop(0, half // CHUNK)
            def _(i):
                inside = pl.multiple_of(i * CHUNK, CHUNK)
                at = pl.ds(h * half + inside, CHUNK)
                acc[a, j, at] += recv[s - 1][slot, h, k, pl.ds(inside, CHUNK)]

    def stage_later(s, p):
        for h in (0, 1):
            for c in stage_copies(s - 1, h, p):
                c.wait()
            add_received(s - 1, h, p)
        for h in (0, 1):
            for c in stage_copies(s, h, p):
                c.start()

    def final_step(p):
        slot, a, m = lax.rem(p, plan.recv_slots[L - 1]), lax.rem(p, plan.acc_slots), (p * R) // rows
        own = plan.first.index(0)
        for h in (0, 1):
            for c in stage_copies(L, h, p):
                c.wait()

            @pl.loop(0, half // CHUNK)
            def _(i):
                inside = pl.multiple_of(i * CHUNK, CHUNK)
                at = h * half + inside
                g = acc[a, own, pl.ds(at, CHUNK)] + recv[L - 1][slot, h, 0, pl.ds(inside, CHUNK)]
                grad[pl.ds(p * R + at, CHUNK)] = g
                q = g * g + tiny_square
                lane = q[:, :LANES]
                for j in range(1, width // LANES):
                    lane = lane + q[:, j * LANES:(j + 1) * LANES]
                row_part[pl.ds(pl.multiple_of(lax.rem(p * R, LANES) + at, CHUNK), CHUNK)] = lane
                col_sum[m] += sum(q[8 * j:8 * j + 8] for j in range(CHUNK // 8))

        last = lax.rem((p + 1) * R, rows) == 0

        @pl.when(last)
        def _():
            col_all[m, my_row] = jnp.sum(col_sum[m], axis=0, keepdims=True)

        @pl.when(lax.rem((p + 1) * R, LANES) == 0)
        def _():
            k = (p * R) // LANES
            row_all[k, me] = jnp.sum(row_part[...].T, axis=0, keepdims=True)

            @pl.when(last)
            def _():
                for i in range(nz - 1, 0, -1):
                    col_copy(m, i).start()

            for r in range(n - 1, 0, -1):
                row_copy(k, r).start()

    def block_step(k):
        m = (k * LANES) // rows
        for r in range(1, n):
            row_arrival(k, r).wait_recv()
        full = row_all[k, 0]
        for c in range(1, n):
            full = full + row_all[k, c]
        fresh = second_decay * row_mine[k] + (1.0 - second_decay) * full / ff
        row_mine[k] = fresh
        nr_sum[m] += fresh
        gain = jnp.broadcast_to(lax.rsqrt(fresh), (LANES, LANES)).T
        for i in range(LANES // 8):
            at = pl.ds(pl.multiple_of(k * LANES + 8 * i, 8), 8)
            by = gain[8 * i:8 * i + 8]
            for j in range(width // LANES):
                lanes = slice(j * LANES, (j + 1) * LANES)
                y = grad[at, lanes] * by
                grad[at, lanes] = y
                w_sum[m, :, lanes] += y * y
        for r in range(1, n):
            row_copy(k, r).wait_send()

    def matrix_step(m):
        for i in range(1, nz):
            col_arrival(m, i).wait_recv()
        full = col_all[m, 0]
        for z in range(1, nz):
            full = full + col_all[m, z]
        fresh = second_decay * col_old[pl.ds(m, 1), :] + (1.0 - second_decay) * full / d
        new_cols[pl.ds(m, 1), :] = fresh
        w = jnp.sum(w_sum[m], axis=0, keepdims=True) / fresh
        part = w[:, :LANES]
        for j in range(1, width // LANES):
            part = part + w[:, j * LANES:(j + 1) * LANES]
        sq_all[m, my_row, me] = jnp.concatenate([part, nr_sum[m]], axis=1)
        for i, r in far:
            sq_copy(m, i, r).start()
        for i in range(1, nz):
            col_copy(m, i).wait_send()

    def scale_step(m):
        for i, r in far:
            sq_arrival(m, i, r).wait_recv()
        both = jnp.sum(sq_all[m].reshape(nz * n, 1, 2 * LANES), axis=0)
        square = jnp.sum(both[:, :LANES], axis=1, keepdims=True)
        mean = jnp.sum(both[:, LANES:], axis=1, keepdims=True) / (n * d)
        clip = jnp.maximum(1.0, jnp.sqrt(square * mean / (d * ff)))
        col_gain[m:m + 1, :] = lax.rsqrt(new_cols[m:m + 1, :]) * (jnp.sqrt(mean) / clip)
        for i, r in far:
            sq_copy(m, i, r).wait_send()

    old_copies = [
        pltpu.make_async_copy(row_moment, row_old, old_sem.at[0]),
        pltpu.make_async_copy(col_moment, col_old, old_sem.at[1]),
    ]

    def old_step():
        for c in old_copies:
            c.wait()
        for m in range(mats):
            for k in range(rows // LANES):
                row_mine[m * (rows // LANES) + k] = row_old[m:m + 1, k * LANES:(k + 1) * LANES]

    o = plan.offset
    load_step(0)
    barrier = pltpu.get_barrier_semaphore()
    partners = [(i, 0) for i in range(nz - 1, 0, -1)] + [(0, bit) for bit in plan.orders[0]]
    for i, r in partners:
        pl.semaphore_signal(barrier, inc=1, device_id={"row": level[i], "col": peer[r]}, device_id_type=MESH)
    for p in range(1, 3):
        load_step(p)
    for c in old_copies:
        c.start()
    nr_sum[...] = jnp.zeros_like(nr_sum)
    col_sum[...] = jnp.zeros_like(col_sum)
    w_sum[...] = jnp.zeros_like(w_sum)
    pl.semaphore_wait(barrier, len(partners))

    per_block = LANES // R
    late = 2

    @pl.loop(-o[0], plan.pieces + 1)
    def _(t):
        def run(p, step):
            pl.when(jnp.logical_and(p >= 0, p < plan.pieces))(lambda: step(p))

        run(t + o[1], stage_one)
        for s in range(2, L + 1):
            run(t + o[s], functools.partial(stage_later, s))
        run(t - 1, final_step)
        run(t + o[0], send_step)
        pl.when(t + o[0] + 3 < plan.pieces)(lambda: load_step(t + o[0] + 3))
        pl.when(t == 0)(old_step)
        done = t - 1 - late

        @pl.when(jnp.logical_and(done >= 0, lax.rem(done + 1, per_block) == 0))
        def _():
            k = done // per_block
            block_step(k)
            pl.when(lax.rem((k + 1) * LANES, rows) == 0)(lambda: matrix_step((k * LANES) // rows))

    seen = plan.pieces - 1 - late
    for k in range((seen + 1) // per_block, plan.blocks):
        block_step(k)
        if (k + 1) * LANES % rows == 0:
            matrix_step(k * LANES // rows)
    for m in range(mats):
        for k in range(rows // LANES):
            new_rows[m:m + 1, k * LANES:(k + 1) * LANES] = row_mine[m * (rows // LANES) + k]
    for p in range(plan.pieces - plan.send_slots, plan.pieces):
        for j in range(n // 2):
            first_copy(p, j).wait_send()
    for m in range(mats):
        scale_step(m)


def finish(mats, grad, col_gain, rows_in, cols_in, update, new_rows, new_cols, scaled, small_sem, out_sem):
    total = grad.shape[0]
    small = [
        pltpu.make_async_copy(rows_in, new_rows, small_sem.at[0]),
        pltpu.make_async_copy(cols_in, new_cols, small_sem.at[1]),
    ]
    step = LANES
    out = [
        pltpu.make_async_copy(scaled.at[pl.ds(c * step, step)], update.at[pl.ds(c * step, step)], out_sem.at[c])
        for c in range(total // step)
    ]
    for c in range(total // step):
        gain = jnp.broadcast_to(col_gain[c * step * mats // total:c * step * mats // total + 1, :], (8, grad.shape[1]))

        @pl.loop(0, step // 8, unroll=2)
        def _(i):
            at = pl.ds(pl.multiple_of(c * step + i * 8, 8), 8)
            scaled[at] = grad[at] * gain

        out[c].start()
        if c == 0:
            for s in small:
                s.start()
    for s in small + out:
        s.wait()


def on_device(n, nz, grad_terms, row_moment, col_moment):
    mats, rows, ff = grad_terms.shape[1:]
    width = ff // n
    d = rows * nz
    plan = Plan(n, nz, mats, rows, width)
    L, R, half = plan.stages, plan.piece, plan.piece // 2
    kept = [len(plan.kept[s][0]) for s in range(L)]
    f32 = jnp.float32
    dma = pltpu.SemaphoreType.DMA
    blocks, total = plan.blocks, mats * rows
    scratch = [
        pltpu.VMEM((plan.load_slots, n, R, width), grad_terms.dtype),
        pltpu.VMEM((plan.send_slots, n // 2, R, width), f32),
        pltpu.VMEM((plan.acc_slots, n // 2, R, width), f32),
        pltpu.VMEM((mats, rows), f32),
        pltpu.VMEM((mats, width), f32),
        pltpu.VMEM((LANES, LANES), f32),
        pltpu.VMEM((blocks, 1, LANES), f32),
        pltpu.VMEM((blocks, n, 1, LANES), f32),
        pltpu.VMEM((mats, 1, LANES), f32),
        pltpu.VMEM((mats, 8, width), f32),
        pltpu.VMEM((mats, 8, width), f32),
        pltpu.VMEM((mats, nz, 1, width), f32),
        pltpu.VMEM((mats, nz, n, 1, 2 * LANES), f32),
        dma((plan.load_slots, n)),
        dma((plan.send_slots, n // 2)),
        dma((plan.acc_slots, n // 2)),
        dma((2,)),
        dma((blocks, n - 1)),
        dma((blocks, n)),
        dma((mats, nz - 1)),
        dma((mats, nz)),
        dma((mats, nz, n)),
        dma((mats, nz, n)),
    ]
    scratch += [pltpu.VMEM((plan.recv_slots[s], 2, kept[s], half, width), f32) for s in range(L)]
    scratch += [dma((plan.recv_slots[s], 2, kept[s])) for s in range(L)] * 2
    vmem, anywhere = pl.BlockSpec(memory_space=pltpu.VMEM), pl.BlockSpec(memory_space=pl.ANY)
    held = pl.pallas_call(
        functools.partial(kernel, plan, ff, d),
        out_shape=(
            pltpu.VMEM((total, width), f32),
            pltpu.VMEM((mats, width), f32),
            pltpu.VMEM((mats, rows), f32),
            pltpu.VMEM((mats, width), f32),
        ),
        in_specs=[anywhere] * 3,
        out_specs=(vmem,) * 4,
        scratch_shapes=scratch,
        compiler_params=pltpu.CompilerParams(
            collective_id=0, has_side_effects=True, vmem_limit_bytes=44 * 1024 * 1024
        ),
        name="reduce_and_level",
    )(grad_terms.reshape(total, ff), row_moment, col_moment)
    update, new_rows, new_cols = pl.pallas_call(
        functools.partial(finish, mats),
        out_shape=(
            jax.ShapeDtypeStruct((total, width), f32),
            jax.ShapeDtypeStruct((mats, rows), f32),
            jax.ShapeDtypeStruct((mats, width), f32),
        ),
        in_specs=[vmem] * 4,
        out_specs=(anywhere,) * 3,
        scratch_shapes=[pltpu.VMEM((total, width), f32), dma((2,)), dma((total // LANES,))],
        compiler_params=pltpu.CompilerParams(vmem_limit_bytes=24 * 1024 * 1024),
        name="scale_and_write",
    )(*held)
    return update.reshape(mats, rows, width), new_rows, new_cols


def solution(mesh):
    n, nz = mesh.shape["col"], mesh.shape["row"]
    return jax.shard_map(
        functools.partial(on_device, n, nz),
        mesh=mesh,
        in_specs=(P("col", None, "row", None), P(None, "row"), P(None, "col")),
        out_specs=(P(None, "row", "col"), P(None, "row"), P(None, "col")),
        check_vma=False,
    )
```

```python
import functools

import jax
import jax.numpy as jnp
from jax import lax
from jax.experimental import pallas as pl
from jax.experimental.pallas import tpu as pltpu
from jax.sharding import PartitionSpec as P

MESH = pl.DeviceIdType.MESH
second_decay = 1.0 - 100.0 ** (-0.8)
tiny_square = 1e-30
LANES = 128
PIECE = 64
CHUNK = 16


def flip(me, r):
    bit = 1
    while bit <= r:
        if r & bit:
            me = me + bit * (1 - 2 * lax.rem(me // bit, 2))
        bit *= 2
    return me


class Plan:
    def __init__(self, n, nz, mats, rows, width):
        bits = [1 << b for b in range(n.bit_length() - 1)]
        self.n, self.nz, self.mats, self.rows, self.width = n, nz, mats, rows, width
        self.orders = (bits, bits[:1] + bits[:0:-1])
        self.stages = len(bits) - 1
        self.first = [r for r in range(n) if not r & bits[0]]
        self.first_bit = bits[0]
        self.kept = []
        self.sent = []
        held = [list(self.first), list(self.first)]
        for s in range(1, self.stages + 1):
            sent = [[r for r in held[h] if r & self.orders[h][s]] for h in (0, 1)]
            held = [[r for r in held[h] if not r & self.orders[h][s]] for h in (0, 1)]
            self.sent.append(sent)
            self.kept.append([list(x) for x in held])
        early = [(r, h) for pair in zip(*(self.sent[0][h][::-1] for h in (0, 1))) for h, r in enumerate(pair)]
        late = [(r, h) for pair in zip(*(self.kept[0][h] for h in (0, 1))) for h, r in enumerate(pair)]
        self.units = early + late
        self.piece = PIECE
        self.pieces = mats * rows // self.piece
        self.blocks = mats * rows // LANES
        L = self.stages
        self.offset = [2 * (L - 1) + 1] + [2 * (L - s) for s in range(1, L + 1)]
        self.acc_slots = self.offset[0] + 4
        self.send_slots = 3
        self.load_slots = 4
        self.recv_slots = [6] * (L - 1) + [4]
        self.row_slots = -(-(self.offset[0] + 4) * self.piece // LANES)


def kernel(plan, ff, d, grad_terms, row_moment, col_moment, grad, col_gain, new_rows, new_cols, *scratch):
    n, nz, mats, rows, width = plan.n, plan.nz, plan.mats, plan.rows, plan.width
    L, R, half = plan.stages, plan.piece, plan.piece // 2
    (loaded, to_send, acc, row_old, col_old, row_part, row_mine, row_all, nr_sum, col_sum, w_sum, col_all, sq_all,
     load_sem, first_send, first_recv, old_sem, row_send, row_recv, col_send, col_recv, sq_send, sq_recv, *rest) = scratch
    recv, send_sem, recv_sem = rest[:L], rest[L:2 * L], rest[2 * L:3 * L]
    me, my_row = lax.axis_index("col"), lax.axis_index("row")
    peer = [flip(me, r) for r in range(n)]
    level = [lax.rem(my_row + i, nz) for i in range(nz)]
    far = [(i, r) for i in range(nz - 1, -1, -1) for r in range(n - 1, -1, -1) if i or r]

    def remote(src, dst, send, rcv, i, r):
        return pltpu.make_async_remote_copy(
            src_ref=src, dst_ref=dst, send_sem=send, recv_sem=rcv,
            device_id={"row": level[i], "col": peer[r]}, device_id_type=MESH,
        )

    def load(p, r):
        slot = lax.rem(p, plan.load_slots)
        at = pl.multiple_of(p * R, R)
        c = pl.multiple_of(peer[r] * width, LANES)
        group = int(r not in plan.first)
        j = plan.first.index(r ^ (group * plan.first_bit))
        return pltpu.make_async_copy(
            grad_terms.at[pl.ds(at, R), pl.ds(c, width)],
            loaded.at[slot, group, j],
            load_sem.at[slot, group],
        )

    def wait_load(p, group):
        slot = lax.rem(p, plan.load_slots)
        both = loaded.at[slot, group]
        pltpu.make_async_copy(both, both, load_sem.at[slot, group]).wait()

    def first_copy(p, r, h):
        a, b, j = lax.rem(p, plan.send_slots), lax.rem(p, plan.acc_slots), plan.first.index(r)
        at = pl.ds(h * half, half)
        return remote(
            to_send.at[a, j, at], acc.at[b, j, at], first_send.at[a], first_recv.at[lax.rem(p, 2), j, h],
            0, plan.first_bit,
        )

    def wait_first_sent(p):
        a = lax.rem(p, plan.send_slots)
        remote(to_send.at[a], to_send.at[a], first_send.at[a], first_recv.at[0, 0, 0], 0, plan.first_bit).wait_send()

    def stage_copy(s, h, p, r):
        slot = lax.rem(p, plan.recv_slots[s - 1])
        bit = plan.orders[h][s]
        j = plan.kept[s - 1][h].index(r ^ bit)
        return remote(
            acc.at[lax.rem(p, plan.acc_slots), plan.first.index(r), pl.ds(h * half, half)],
            recv[s - 1].at[slot, h, j],
            send_sem[s - 1].at[slot, h],
            recv_sem[s - 1].at[slot, h],
            0,
            bit,
        )

    def wait_stage(s, h, p):
        slot = lax.rem(p, plan.recv_slots[s - 1])
        both = recv[s - 1].at[slot, h]
        remote(both, both, send_sem[s - 1].at[slot, h], recv_sem[s - 1].at[slot, h], 0, plan.orders[h][s]).wait()

    def row_copy(k, r):
        at = lax.rem(k, plan.row_slots)
        return remote(row_all.at[k, me], row_all.at[k, me], row_send.at[at], row_recv.at[at], 0, r)

    def row_group(k):
        at, others = lax.rem(k, plan.row_slots), row_all.at[k, pl.ds(0, n - 1)]
        return remote(others, others, row_send.at[at], row_recv.at[at], 0, 1)

    def col_copy(m, i):
        return remote(col_all.at[m, my_row], col_all.at[m, my_row], col_send.at[m], col_recv.at[m], i, 0)

    def col_group(m):
        others = col_all.at[m, pl.ds(0, nz - 1)]
        return remote(others, others, col_send.at[m], col_recv.at[m], 1, 0)

    def sq_copy(m, i, r):
        here = sq_all.at[m, my_row * n + me]
        return remote(here, here, sq_send.at[m], sq_recv.at[m], i, r)

    def sq_group(m):
        others = sq_all.at[m, pl.ds(0, nz * n - 1)]
        return remote(others, others, sq_send.at[m], sq_recv.at[m], 1, 0)

    def load_step(p):
        for r in plan.first:
            load(p, r ^ plan.first_bit).start()
        for r in plan.first:
            load(p, r).start()

    def send_step(p):
        slot, into = lax.rem(p, plan.load_slots), lax.rem(p, plan.send_slots)
        pl.when(p >= plan.send_slots)(lambda: wait_first_sent(p - plan.send_slots))
        wait_load(p, 1)
        for r, h in plan.units:
            j = plan.first.index(r)

            @pl.loop(0, half // CHUNK)
            def _(i):
                at = pl.ds(pl.multiple_of(h * half + i * CHUNK, CHUNK), CHUNK)
                to_send[into, j, at] = loaded[slot, 1, j, at].astype(jnp.float32)

            first_copy(p, r, h).start()

    def stage_one(p):
        slot, a = lax.rem(p, plan.load_slots), lax.rem(p, plan.acc_slots)
        wait_load(p, 0)
        for r, h in plan.units:
            j = plan.first.index(r)
            first_copy(p, r, h).wait_recv()

            @pl.loop(0, half // CHUNK)
            def _(i):
                at = pl.ds(pl.multiple_of(h * half + i * CHUNK, CHUNK), CHUNK)
                acc[a, j, at] += loaded[slot, 0, j, at].astype(jnp.float32)

            if r in plan.sent[0][h]:
                stage_copy(1, h, p, r).start()

    def add_received(s, h, p):
        slot, a = lax.rem(p, plan.recv_slots[s - 1]), lax.rem(p, plan.acc_slots)
        for k, r in enumerate(plan.kept[s - 1][h]):
            j = plan.first.index(r)

            @pl.loop(0, half // CHUNK)
            def _(i):
                inside = pl.multiple_of(i * CHUNK, CHUNK)
                at = pl.ds(h * half + inside, CHUNK)
                acc[a, j, at] += recv[s - 1][slot, h, k, pl.ds(inside, CHUNK)]

    def stage_later(s, p):
        for h in (0, 1):
            wait_stage(s - 1, h, p)
            add_received(s - 1, h, p)
        for h in (0, 1):
            for r in plan.sent[s - 1][h]:
                stage_copy(s, h, p, r).start()

    def final_step(p):
        slot, a, m = lax.rem(p, plan.recv_slots[L - 1]), lax.rem(p, plan.acc_slots), (p * R) // rows
        own = plan.first.index(0)
        for h in (0, 1):
            wait_stage(L, h, p)

            @pl.loop(0, half // CHUNK)
            def _(i):
                inside = pl.multiple_of(i * CHUNK, CHUNK)
                at = h * half + inside
                g = acc[a, own, pl.ds(at, CHUNK)] + recv[L - 1][slot, h, 0, pl.ds(inside, CHUNK)]
                grad[pl.ds(p * R + at, CHUNK)] = g
                q = g * g + tiny_square
                lane = q[:, :LANES]
                for j in range(1, width // LANES):
                    lane = lane + q[:, j * LANES:(j + 1) * LANES]
                row_part[pl.ds(pl.multiple_of(lax.rem(p * R, LANES) + at, CHUNK), CHUNK)] = lane
                col_sum[m] += sum(q[8 * j:8 * j + 8] for j in range(CHUNK // 8))

        last = lax.rem((p + 1) * R, rows) == 0

        @pl.when(last)
        def _():
            col_all[m, my_row] = jnp.sum(col_sum[m], axis=0, keepdims=True)

        @pl.when(lax.rem((p + 1) * R, LANES) == 0)
        def _():
            k = (p * R) // LANES
            row_all[k, me] = jnp.sum(row_part[...].T, axis=0, keepdims=True)

            @pl.when(last)
            def _():
                for i in range(nz - 1, 0, -1):
                    col_copy(m, i).start()

            for r in range(n - 1, 0, -1):
                row_copy(k, r).start()

    def block_step(k):
        m = (k * LANES) // rows
        row_group(k).wait_recv()
        full = row_all[k, 0]
        for c in range(1, n):
            full = full + row_all[k, c]
        fresh = second_decay * row_mine[k] + (1.0 - second_decay) * full / ff
        row_mine[k] = fresh
        nr_sum[m] += fresh
        gain = jnp.broadcast_to(lax.rsqrt(fresh), (LANES, LANES)).T
        for i in range(LANES // 8):
            at = pl.ds(pl.multiple_of(k * LANES + 8 * i, 8), 8)
            by = gain[8 * i:8 * i + 8]
            for j in range(width // LANES):
                lanes = slice(j * LANES, (j + 1) * LANES)
                y = grad[at, lanes] * by
                grad[at, lanes] = y
                w_sum[m, :, lanes] += y * y
        row_group(k).wait_send()

    def matrix_step(m):
        col_group(m).wait_recv()
        full = col_all[m, 0]
        for z in range(1, nz):
            full = full + col_all[m, z]
        fresh = second_decay * col_old[pl.ds(m, 1), :] + (1.0 - second_decay) * full / d
        new_cols[pl.ds(m, 1), :] = fresh
        w = jnp.sum(w_sum[m], axis=0, keepdims=True) / fresh
        part = w[:, :LANES]
        for j in range(1, width // LANES):
            part = part + w[:, j * LANES:(j + 1) * LANES]
        sq_all[m, my_row * n + me] = jnp.concatenate([part, nr_sum[m]], axis=1)
        for i, r in far:
            sq_copy(m, i, r).start()
        col_group(m).wait_send()

    def scale_step(m):
        sq_group(m).wait_recv()
        both = jnp.sum(sq_all[m], axis=0)
        square = jnp.sum(both[:, :LANES], axis=1, keepdims=True)
        mean = jnp.sum(both[:, LANES:], axis=1, keepdims=True) / (n * d)
        clip = jnp.maximum(1.0, jnp.sqrt(square * mean / (d * ff)))
        col_gain[m:m + 1, :] = lax.rsqrt(new_cols[m:m + 1, :]) * (jnp.sqrt(mean) / clip)
        sq_group(m).wait_send()

    old_copies = [
        pltpu.make_async_copy(row_moment, row_old, old_sem.at[0]),
        pltpu.make_async_copy(col_moment, col_old, old_sem.at[1]),
    ]

    def old_step():
        for c in old_copies:
            c.wait()
        for m in range(mats):
            for k in range(rows // LANES):
                row_mine[m * (rows // LANES) + k] = row_old[m:m + 1, k * LANES:(k + 1) * LANES]

    o = plan.offset
    load_step(0)
    barrier = pltpu.get_barrier_semaphore()
    partners = [(i, 0) for i in range(nz - 1, 0, -1)] + [(0, bit) for bit in plan.orders[0]]
    for i, r in partners:
        pl.semaphore_signal(barrier, inc=1, device_id={"row": level[i], "col": peer[r]}, device_id_type=MESH)
    for p in range(1, 3):
        load_step(p)
    for c in old_copies:
        c.start()
    nr_sum[...] = jnp.zeros_like(nr_sum)
    col_sum[...] = jnp.zeros_like(col_sum)
    w_sum[...] = jnp.zeros_like(w_sum)
    pl.semaphore_wait(barrier, len(partners))

    per_block = LANES // R
    late = 2

    @pl.loop(-o[0], plan.pieces + 1)
    def _(t):
        def run(p, step):
            pl.when(jnp.logical_and(p >= 0, p < plan.pieces))(lambda: step(p))

        run(t + o[1], stage_one)
        for s in range(2, L + 1):
            run(t + o[s], functools.partial(stage_later, s))
        run(t - 1, final_step)
        run(t + o[0], send_step)
        pl.when(t + o[0] + 3 < plan.pieces)(lambda: load_step(t + o[0] + 3))
        pl.when(t == 0)(old_step)
        done = t - 1 - late

        @pl.when(jnp.logical_and(done >= 0, lax.rem(done + 1, per_block) == 0))
        def _():
            k = done // per_block
            block_step(k)
            pl.when(lax.rem((k + 1) * LANES, rows) == 0)(lambda: matrix_step((k * LANES) // rows))

    seen = plan.pieces - 1 - late
    for k in range((seen + 1) // per_block, plan.blocks):
        block_step(k)
        if (k + 1) * LANES % rows == 0:
            matrix_step(k * LANES // rows)
    for m in range(mats):
        for k in range(rows // LANES):
            new_rows[m:m + 1, k * LANES:(k + 1) * LANES] = row_mine[m * (rows // LANES) + k]
    for p in range(plan.pieces - plan.send_slots, plan.pieces):
        wait_first_sent(p)
    for m in range(mats):
        scale_step(m)


def finish(mats, grad, col_gain, rows_in, cols_in, update, new_rows, new_cols, scaled, small_sem, out_sem):
    total = grad.shape[0]
    small = [
        pltpu.make_async_copy(rows_in, new_rows, small_sem.at[0]),
        pltpu.make_async_copy(cols_in, new_cols, small_sem.at[1]),
    ]
    step = LANES
    out = [
        pltpu.make_async_copy(scaled.at[pl.ds(c * step, step)], update.at[pl.ds(c * step, step)], out_sem)
        for c in range(total // step)
    ]
    for c in range(total // step):
        gain = jnp.broadcast_to(col_gain[c * step * mats // total:c * step * mats // total + 1, :], (8, grad.shape[1]))

        @pl.loop(0, step // 8, unroll=2)
        def _(i):
            at = pl.ds(pl.multiple_of(c * step + i * 8, 8), 8)
            scaled[at] = grad[at] * gain

        out[c].start()
        if c == 0:
            for s in small:
                s.start()
    for s in small:
        s.wait()
    pltpu.make_async_copy(scaled, update, out_sem).wait()


def on_device(n, nz, grad_terms, row_moment, col_moment):
    mats, rows, ff = grad_terms.shape[1:]
    width = ff // n
    d = rows * nz
    plan = Plan(n, nz, mats, rows, width)
    L, R, half, everyone = plan.stages, plan.piece, plan.piece // 2, n * nz
    kept = [len(plan.kept[s][0]) for s in range(L)]
    f32 = jnp.float32
    dma = pltpu.SemaphoreType.DMA
    blocks, total = plan.blocks, mats * rows
    scratch = [
        pltpu.VMEM((plan.load_slots, 2, n // 2, R, width), grad_terms.dtype),
        pltpu.VMEM((plan.send_slots, n // 2, R, width), f32),
        pltpu.VMEM((plan.acc_slots, n // 2, R, width), f32),
        pltpu.VMEM((mats, rows), f32),
        pltpu.VMEM((mats, width), f32),
        pltpu.VMEM((LANES, LANES), f32),
        pltpu.VMEM((blocks, 1, LANES), f32),
        pltpu.VMEM((blocks, n, 1, LANES), f32),
        pltpu.VMEM((mats, 1, LANES), f32),
        pltpu.VMEM((mats, 8, width), f32),
        pltpu.VMEM((mats, 8, width), f32),
        pltpu.VMEM((mats, nz, 1, width), f32),
        pltpu.VMEM((mats, everyone, 1, 2 * LANES), f32),
        dma((plan.load_slots, 2)),
        dma((plan.send_slots,)),
        dma((2, n // 2, 2)),
        dma((2,)),
        dma((plan.row_slots,)),
        dma((plan.row_slots,)),
        dma((mats,)),
        dma((mats,)),
        dma((mats,)),
        dma((mats,)),
    ]
    scratch += [pltpu.VMEM((plan.recv_slots[s], 2, kept[s], half, width), f32) for s in range(L)]
    scratch += [dma((plan.recv_slots[s], 2)) for s in range(L)] * 2
    vmem, anywhere = pl.BlockSpec(memory_space=pltpu.VMEM), pl.BlockSpec(memory_space=pl.ANY)
    held = pl.pallas_call(
        functools.partial(kernel, plan, ff, d),
        out_shape=(
            pltpu.VMEM((total, width), f32),
            pltpu.VMEM((mats, width), f32),
            pltpu.VMEM((mats, rows), f32),
            pltpu.VMEM((mats, width), f32),
        ),
        in_specs=[anywhere] * 3,
        out_specs=(vmem,) * 4,
        scratch_shapes=scratch,
        compiler_params=pltpu.CompilerParams(
            collective_id=0, has_side_effects=True, vmem_limit_bytes=44 * 1024 * 1024
        ),
        name="reduce_and_level",
    )(grad_terms.reshape(total, ff), row_moment, col_moment)
    update, new_rows, new_cols = pl.pallas_call(
        functools.partial(finish, mats),
        out_shape=(
            jax.ShapeDtypeStruct((total, width), f32),
            jax.ShapeDtypeStruct((mats, rows), f32),
            jax.ShapeDtypeStruct((mats, width), f32),
        ),
        in_specs=[vmem] * 4,
        out_specs=(anywhere,) * 3,
        scratch_shapes=[pltpu.VMEM((total, width), f32), dma((2,)), dma],
        compiler_params=pltpu.CompilerParams(vmem_limit_bytes=24 * 1024 * 1024),
        name="scale_and_write",
    )(*held)
    return update.reshape(mats, rows, width), new_rows, new_cols


def solution(mesh):
    n, nz = mesh.shape["col"], mesh.shape["row"]
    return jax.shard_map(
        functools.partial(on_device, n, nz),
        mesh=mesh,
        in_specs=(P("col", None, "row", None), P(None, "row"), P(None, "col")),
        out_specs=(P(None, "row", "col"), P(None, "row"), P(None, "col")),
        check_vma=False,
    )
```

```python
import functools

import jax
import jax.numpy as jnp
from jax import lax
from jax.experimental import pallas as pl
from jax.experimental.pallas import tpu as pltpu
from jax.sharding import PartitionSpec as P

MESH = pl.DeviceIdType.MESH
second_decay = 1.0 - 100.0 ** (-0.8)
tiny_square = 1e-30
LANES = 128
PIECE = 64
CHUNK = 16


def flip(me, r):
    bit = 1
    while bit <= r:
        if r & bit:
            me = me + bit * (1 - 2 * lax.rem(me // bit, 2))
        bit *= 2
    return me


class Plan:
    def __init__(self, n, nz, mats, rows, width):
        bits = [1 << b for b in range(n.bit_length() - 1)]
        self.n, self.nz, self.mats, self.rows, self.width = n, nz, mats, rows, width
        self.orders = (bits, bits[:1] + bits[:0:-1])
        self.stages = len(bits) - 1
        self.first = [r for r in range(n) if not r & bits[0]]
        self.first_bit = bits[0]
        self.kept = []
        self.sent = []
        held = [list(self.first), list(self.first)]
        for s in range(1, self.stages + 1):
            sent = [[r for r in held[h] if r & self.orders[h][s]] for h in (0, 1)]
            held = [[r for r in held[h] if not r & self.orders[h][s]] for h in (0, 1)]
            self.sent.append(sent)
            self.kept.append([list(x) for x in held])
        early = [(r, h) for pair in zip(*(self.sent[0][h][::-1] for h in (0, 1))) for h, r in enumerate(pair)]
        late = [(r, h) for pair in zip(*(self.kept[0][h] for h in (0, 1))) for h, r in enumerate(pair)]
        self.units = early + late
        self.piece = PIECE
        self.pieces = mats * rows // self.piece
        self.blocks = mats * rows // LANES
        L = self.stages
        self.offset = [2 * (L - 1) + 1] + [2 * (L - s) for s in range(1, L + 1)]
        self.acc_slots = self.offset[0] + 4
        self.send_slots = 3
        self.load_slots = 4
        self.recv_slots = [6] * (L - 1) + [4]
        self.row_slots = -(-(self.offset[0] + 4) * self.piece // LANES)


def kernel(plan, ff, d, grad_terms, row_moment, col_moment, grad, col_gain, new_rows, new_cols, *scratch):
    n, nz, mats, rows, width = plan.n, plan.nz, plan.mats, plan.rows, plan.width
    L, R, half = plan.stages, plan.piece, plan.piece // 2
    (loaded, to_send, acc, row_old, col_old, row_part, row_mine, row_all, nr_sum, col_sum, w_sum, col_all, sq_all,
     load_sem, first_send, first_recv, old_sem, row_send, row_recv, col_send, col_recv, sq_send, sq_recv, *rest) = scratch
    recv, send_sem, recv_sem = rest[:L], rest[L:2 * L], rest[2 * L:3 * L]
    me, my_row = lax.axis_index("col"), lax.axis_index("row")
    peer = [flip(me, r) for r in range(n)]
    level = [lax.rem(my_row + i, nz) for i in range(nz)]
    far = [(i, r) for i in range(nz - 1, -1, -1) for r in range(n - 1, -1, -1) if i or r]

    def remote(src, dst, send, rcv, i, r):
        return pltpu.make_async_remote_copy(
            src_ref=src, dst_ref=dst, send_sem=send, recv_sem=rcv,
            device_id={"row": level[i], "col": peer[r]}, device_id_type=MESH,
        )

    def load(p, r):
        slot = lax.rem(p, plan.load_slots)
        at = pl.multiple_of(p * R, R)
        c = pl.multiple_of(peer[r] * width, LANES)
        group = int(r not in plan.first)
        j = plan.first.index(r ^ (group * plan.first_bit))
        return pltpu.make_async_copy(
            grad_terms.at[pl.ds(at, R), pl.ds(c, width)],
            loaded.at[slot, group, j],
            load_sem.at[slot, group],
        )

    def wait_load(p, group):
        slot = lax.rem(p, plan.load_slots)
        both = loaded.at[slot, group]
        pltpu.make_async_copy(both, both, load_sem.at[slot, group]).wait()

    def first_copy(p, r, h):
        a, b, j = lax.rem(p, plan.send_slots), lax.rem(p, plan.acc_slots), plan.first.index(r)
        at = pl.ds(h * half, half)
        return remote(
            to_send.at[a, j, at], acc.at[b, j, at], first_send.at[a], first_recv.at[lax.rem(p, 2), j, h],
            0, plan.first_bit,
        )

    def wait_first_sent(p):
        a = lax.rem(p, plan.send_slots)
        remote(to_send.at[a], to_send.at[a], first_send.at[a], first_recv.at[0, 0, 0], 0, plan.first_bit).wait_send()

    def stage_copy(s, h, p, r):
        slot = lax.rem(p, plan.recv_slots[s - 1])
        bit = plan.orders[h][s]
        j = plan.kept[s - 1][h].index(r ^ bit)
        return remote(
            acc.at[lax.rem(p, plan.acc_slots), plan.first.index(r), pl.ds(h * half, half)],
            recv[s - 1].at[slot, h, j],
            send_sem[s - 1].at[slot],
            recv_sem[s - 1].at[slot],
            0,
            bit,
        )

    def wait_stage(s, p):
        slot = lax.rem(p, plan.recv_slots[s - 1])
        both = recv[s - 1].at[slot]
        remote(both, both, send_sem[s - 1].at[slot], recv_sem[s - 1].at[slot], 0, plan.orders[0][s]).wait()

    def row_copy(k, r):
        at = lax.rem(k, plan.row_slots)
        return remote(row_all.at[k, me], row_all.at[k, me], row_send.at[at], row_recv.at[at], 0, r)

    def row_group(k):
        at, others = lax.rem(k, plan.row_slots), row_all.at[k, pl.ds(0, n - 1)]
        return remote(others, others, row_send.at[at], row_recv.at[at], 0, 1)

    def col_copy(m, i):
        return remote(col_all.at[m, my_row], col_all.at[m, my_row], col_send.at[m], col_recv.at[m], i, 0)

    def col_group(m):
        others = col_all.at[m, pl.ds(0, nz - 1)]
        return remote(others, others, col_send.at[m], col_recv.at[m], 1, 0)

    def sq_copy(m, i, r):
        here = sq_all.at[m, my_row * n + me]
        return remote(here, here, sq_send.at[m], sq_recv.at[m], i, r)

    def sq_group(m):
        others = sq_all.at[m, pl.ds(0, nz * n - 1)]
        return remote(others, others, sq_send.at[m], sq_recv.at[m], 1, 0)

    def load_step(p):
        for r in plan.first:
            load(p, r ^ plan.first_bit).start()
        for r in plan.first:
            load(p, r).start()

    def send_step(p):
        slot, into = lax.rem(p, plan.load_slots), lax.rem(p, plan.send_slots)
        pl.when(p >= plan.send_slots)(lambda: wait_first_sent(p - plan.send_slots))
        wait_load(p, 1)
        for r, h in plan.units:
            j = plan.first.index(r)

            @pl.loop(0, half // CHUNK)
            def _(i):
                at = pl.ds(pl.multiple_of(h * half + i * CHUNK, CHUNK), CHUNK)
                to_send[into, j, at] = loaded[slot, 1, j, at].astype(jnp.float32)

            first_copy(p, r, h).start()

    def stage_one(p):
        slot, a = lax.rem(p, plan.load_slots), lax.rem(p, plan.acc_slots)
        wait_load(p, 0)
        for r, h in plan.units:
            j = plan.first.index(r)
            first_copy(p, r, h).wait_recv()

            @pl.loop(0, half // CHUNK)
            def _(i):
                at = pl.ds(pl.multiple_of(h * half + i * CHUNK, CHUNK), CHUNK)
                acc[a, j, at] += loaded[slot, 0, j, at].astype(jnp.float32)

            if r in plan.sent[0][h]:
                stage_copy(1, h, p, r).start()

    def add_received(s, h, p):
        slot, a = lax.rem(p, plan.recv_slots[s - 1]), lax.rem(p, plan.acc_slots)
        for k, r in enumerate(plan.kept[s - 1][h]):
            j = plan.first.index(r)

            @pl.loop(0, half // CHUNK)
            def _(i):
                inside = pl.multiple_of(i * CHUNK, CHUNK)
                at = pl.ds(h * half + inside, CHUNK)
                acc[a, j, at] += recv[s - 1][slot, h, k, pl.ds(inside, CHUNK)]

    def stage_later(s, p):
        wait_stage(s - 1, p)
        for h in (0, 1):
            add_received(s - 1, h, p)
        for h in (0, 1):
            for r in plan.sent[s - 1][h]:
                stage_copy(s, h, p, r).start()

    def final_step(p):
        slot, a, m = lax.rem(p, plan.recv_slots[L - 1]), lax.rem(p, plan.acc_slots), (p * R) // rows
        own = plan.first.index(0)
        wait_stage(L, p)
        for h in (0, 1):

            @pl.loop(0, half // CHUNK)
            def _(i):
                inside = pl.multiple_of(i * CHUNK, CHUNK)
                at = h * half + inside
                g = acc[a, own, pl.ds(at, CHUNK)] + recv[L - 1][slot, h, 0, pl.ds(inside, CHUNK)]
                grad[pl.ds(p * R + at, CHUNK)] = g
                q = g * g + tiny_square
                lane = q[:, :LANES]
                for j in range(1, width // LANES):
                    lane = lane + q[:, j * LANES:(j + 1) * LANES]
                row_part[pl.ds(pl.multiple_of(lax.rem(p * R, LANES) + at, CHUNK), CHUNK)] = lane
                col_sum[m] += sum(q[8 * j:8 * j + 8] for j in range(CHUNK // 8))

        last = lax.rem((p + 1) * R, rows) == 0

        @pl.when(last)
        def _():
            col_all[m, my_row] = jnp.sum(col_sum[m], axis=0, keepdims=True)
            for i in range(nz - 1, 0, -1):
                col_copy(m, i).start()

        @pl.when(lax.rem((p + 1) * R, LANES) == 0)
        def _():
            k = (p * R) // LANES
            row_all[k, me] = jnp.sum(row_part[...].T, axis=0, keepdims=True)
            for r in range(n - 1, 0, -1):
                row_copy(k, r).start()

    def block_step(k):
        m = (k * LANES) // rows
        row_group(k).wait_recv()
        full = row_all[k, 0]
        for c in range(1, n):
            full = full + row_all[k, c]
        fresh = second_decay * row_mine[k] + (1.0 - second_decay) * full / ff
        row_mine[k] = fresh
        nr_sum[m] += fresh
        gain = jnp.broadcast_to(lax.rsqrt(fresh), (LANES, LANES)).T
        for i in range(LANES // 8):
            at = pl.ds(pl.multiple_of(k * LANES + 8 * i, 8), 8)
            by = gain[8 * i:8 * i + 8]
            for j in range(width // LANES):
                lanes = slice(j * LANES, (j + 1) * LANES)
                y = grad[at, lanes] * by
                grad[at, lanes] = y
                w_sum[m, :, lanes] += y * y
        row_group(k).wait_send()

    def matrix_step(m):
        col_group(m).wait_recv()
        full = col_all[m, 0]
        for z in range(1, nz):
            full = full + col_all[m, z]
        fresh = second_decay * col_old[pl.ds(m, 1), :] + (1.0 - second_decay) * full / d
        new_cols[pl.ds(m, 1), :] = fresh
        w = jnp.sum(w_sum[m], axis=0, keepdims=True) / fresh
        part = w[:, :LANES]
        for j in range(1, width // LANES):
            part = part + w[:, j * LANES:(j + 1) * LANES]
        sq_all[m, my_row * n + me] = jnp.concatenate([part, nr_sum[m]], axis=1)
        for i, r in far:
            sq_copy(m, i, r).start()
        col_group(m).wait_send()

    def scale_step(m):
        sq_group(m).wait_recv()
        both = jnp.sum(sq_all[m], axis=0)
        square = jnp.sum(both[:, :LANES], axis=1, keepdims=True)
        mean = jnp.sum(both[:, LANES:], axis=1, keepdims=True) / (n * d)
        clip = jnp.maximum(1.0, jnp.sqrt(square * mean / (d * ff)))
        col_gain[m:m + 1, :] = lax.rsqrt(new_cols[m:m + 1, :]) * (jnp.sqrt(mean) / clip)
        sq_group(m).wait_send()

    old_copies = [
        pltpu.make_async_copy(row_moment, row_old, old_sem.at[0]),
        pltpu.make_async_copy(col_moment, col_old, old_sem.at[1]),
    ]

    def old_step():
        for c in old_copies:
            c.wait()
        for m in range(mats):
            for k in range(rows // LANES):
                row_mine[m * (rows // LANES) + k] = row_old[m:m + 1, k * LANES:(k + 1) * LANES]

    o = plan.offset
    load_step(0)
    barrier = pltpu.get_barrier_semaphore()
    partners = [(i, 0) for i in range(nz - 1, 0, -1)] + [(0, bit) for bit in plan.orders[0]]
    for i, r in partners:
        pl.semaphore_signal(barrier, inc=1, device_id={"row": level[i], "col": peer[r]}, device_id_type=MESH)
    for p in range(1, 3):
        load_step(p)
    for c in old_copies:
        c.start()
    nr_sum[...] = jnp.zeros_like(nr_sum)
    col_sum[...] = jnp.zeros_like(col_sum)
    w_sum[...] = jnp.zeros_like(w_sum)
    pl.semaphore_wait(barrier, len(partners))

    per_block = LANES // R
    late = 2

    @pl.loop(-o[0], plan.pieces + 1)
    def _(t):
        def run(p, step):
            pl.when(jnp.logical_and(p >= 0, p < plan.pieces))(lambda: step(p))

        run(t + o[1], stage_one)
        for s in range(2, L + 1):
            run(t + o[s], functools.partial(stage_later, s))
        run(t - 1, final_step)
        run(t + o[0], send_step)
        pl.when(t + o[0] + 3 < plan.pieces)(lambda: load_step(t + o[0] + 3))
        pl.when(t == 0)(old_step)
        done = t - 1 - late

        @pl.when(jnp.logical_and(done >= 0, lax.rem(done + 1, per_block) == 0))
        def _():
            k = done // per_block
            block_step(k)
            pl.when(lax.rem((k + 1) * LANES, rows) == 0)(lambda: matrix_step((k * LANES) // rows))

    seen = plan.pieces - 1 - late
    for k in range((seen + 1) // per_block, plan.blocks):
        block_step(k)
        if (k + 1) * LANES % rows == 0:
            matrix_step(k * LANES // rows)
    for m in range(mats):
        for k in range(rows // LANES):
            new_rows[m:m + 1, k * LANES:(k + 1) * LANES] = row_mine[m * (rows // LANES) + k]
    for p in range(plan.pieces - plan.send_slots, plan.pieces):
        wait_first_sent(p)
    for m in range(mats):
        scale_step(m)


def finish(mats, grad, col_gain, rows_in, cols_in, update, new_rows, new_cols, scaled, small_sem, out_sem):
    total = grad.shape[0]
    small = [
        pltpu.make_async_copy(rows_in, new_rows, small_sem.at[0]),
        pltpu.make_async_copy(cols_in, new_cols, small_sem.at[1]),
    ]
    step = LANES // 2
    out = [
        pltpu.make_async_copy(scaled.at[pl.ds(c * step, step)], update.at[pl.ds(c * step, step)], out_sem)
        for c in range(total // step)
    ]
    for c in range(total // step):
        gain = jnp.broadcast_to(col_gain[c * step * mats // total:c * step * mats // total + 1, :], (8, grad.shape[1]))

        @pl.loop(0, step // 8, unroll=2)
        def _(i):
            at = pl.ds(pl.multiple_of(c * step + i * 8, 8), 8)
            scaled[at] = grad[at] * gain

        out[c].start()
        if c == 0:
            for s in small:
                s.start()
    for s in small:
        s.wait()
    pltpu.make_async_copy(scaled, update, out_sem).wait()


def on_device(n, nz, grad_terms, row_moment, col_moment):
    mats, rows, ff = grad_terms.shape[1:]
    width = ff // n
    d = rows * nz
    plan = Plan(n, nz, mats, rows, width)
    L, R, half, everyone = plan.stages, plan.piece, plan.piece // 2, n * nz
    kept = [len(plan.kept[s][0]) for s in range(L)]
    f32 = jnp.float32
    dma = pltpu.SemaphoreType.DMA
    blocks, total = plan.blocks, mats * rows
    scratch = [
        pltpu.VMEM((plan.load_slots, 2, n // 2, R, width), grad_terms.dtype),
        pltpu.VMEM((plan.send_slots, n // 2, R, width), f32),
        pltpu.VMEM((plan.acc_slots, n // 2, R, width), f32),
        pltpu.VMEM((mats, rows), f32),
        pltpu.VMEM((mats, width), f32),
        pltpu.VMEM((LANES, LANES), f32),
        pltpu.VMEM((blocks, 1, LANES), f32),
        pltpu.VMEM((blocks, n, 1, LANES), f32),
        pltpu.VMEM((mats, 1, LANES), f32),
        pltpu.VMEM((mats, 8, width), f32),
        pltpu.VMEM((mats, 8, width), f32),
        pltpu.VMEM((mats, nz, 1, width), f32),
        pltpu.VMEM((mats, everyone, 1, 2 * LANES), f32),
        dma((plan.load_slots, 2)),
        dma((plan.send_slots,)),
        dma((2, n // 2, 2)),
        dma((2,)),
        dma((plan.row_slots,)),
        dma((plan.row_slots,)),
        dma((mats,)),
        dma((mats,)),
        dma((mats,)),
        dma((mats,)),
    ]
    scratch += [pltpu.VMEM((plan.recv_slots[s], 2, kept[s], half, width), f32) for s in range(L)]
    scratch += [dma((plan.recv_slots[s],)) for s in range(L)] * 2
    vmem, anywhere = pl.BlockSpec(memory_space=pltpu.VMEM), pl.BlockSpec(memory_space=pl.ANY)
    held = pl.pallas_call(
        functools.partial(kernel, plan, ff, d),
        out_shape=(
            pltpu.VMEM((total, width), f32),
            pltpu.VMEM((mats, width), f32),
            pltpu.VMEM((mats, rows), f32),
            pltpu.VMEM((mats, width), f32),
        ),
        in_specs=[anywhere] * 3,
        out_specs=(vmem,) * 4,
        scratch_shapes=scratch,
        compiler_params=pltpu.CompilerParams(
            collective_id=0, has_side_effects=True, vmem_limit_bytes=44 * 1024 * 1024
        ),
        name="reduce_and_level",
    )(grad_terms.reshape(total, ff), row_moment, col_moment)
    update, new_rows, new_cols = pl.pallas_call(
        functools.partial(finish, mats),
        out_shape=(
            jax.ShapeDtypeStruct((total, width), f32),
            jax.ShapeDtypeStruct((mats, rows), f32),
            jax.ShapeDtypeStruct((mats, width), f32),
        ),
        in_specs=[vmem] * 4,
        out_specs=(anywhere,) * 3,
        scratch_shapes=[pltpu.VMEM((total, width), f32), dma((2,)), dma],
        compiler_params=pltpu.CompilerParams(vmem_limit_bytes=24 * 1024 * 1024),
        name="scale_and_write",
    )(*held)
    return update.reshape(mats, rows, width), new_rows, new_cols


def solution(mesh):
    n, nz = mesh.shape["col"], mesh.shape["row"]
    return jax.shard_map(
        functools.partial(on_device, n, nz),
        mesh=mesh,
        in_specs=(P("col", None, "row", None), P(None, "row"), P(None, "col")),
        out_specs=(P(None, "row", "col"), P(None, "row"), P(None, "col")),
        check_vma=False,
    )
```

```python
import functools

import jax
import jax.numpy as jnp
from jax import lax
from jax.experimental import pallas as pl
from jax.experimental.pallas import tpu as pltpu
from jax.sharding import PartitionSpec as P

MESH = pl.DeviceIdType.MESH
second_decay = 1.0 - 100.0 ** (-0.8)
tiny_square = 1e-30
LANES = 128
PIECE = 64
CHUNK = 16


def flip(me, r):
    bit = 1
    while bit <= r:
        if r & bit:
            me = me + bit * (1 - 2 * lax.rem(me // bit, 2))
        bit *= 2
    return me


class Plan:
    def __init__(self, n, nz, mats, rows, width):
        bits = [1 << b for b in range(n.bit_length() - 1)]
        self.n, self.nz, self.mats, self.rows, self.width = n, nz, mats, rows, width
        self.orders = (bits, bits[:1] + bits[:0:-1])
        self.stages = len(bits) - 1
        self.first = [r for r in range(n) if not r & bits[0]]
        self.first_bit = bits[0]
        self.kept = []
        self.sent = []
        held = [list(self.first), list(self.first)]
        for s in range(1, self.stages + 1):
            sent = [[r for r in held[h] if r & self.orders[h][s]] for h in (0, 1)]
            held = [[r for r in held[h] if not r & self.orders[h][s]] for h in (0, 1)]
            self.sent.append(sent)
            self.kept.append([list(x) for x in held])
        early = [(r, h) for pair in zip(*(self.sent[0][h][::-1] for h in (0, 1))) for h, r in enumerate(pair)]
        late = [(r, h) for pair in zip(*(self.kept[0][h] for h in (0, 1))) for h, r in enumerate(pair)]
        self.units = early + late
        self.piece = PIECE
        self.pieces = mats * rows // self.piece
        self.blocks = mats * rows // LANES
        L = self.stages
        self.offset = [2 * (L - 1) + 1] + [2 * (L - s) for s in range(1, L + 1)]
        self.acc_slots = self.offset[0] + 4
        self.send_slots = 3
        self.load_slots = 3
        self.recv_slots = [6] * (L - 1) + [4]
        self.flight = lambda s: 3 if s < L else 2
        self.row_slots = -(-(self.offset[0] + 4) * self.piece // LANES)


def kernel(plan, ff, d, grad_terms, row_moment, col_moment, grad, col_gain, new_rows, new_cols, *scratch):
    n, nz, mats, rows, width = plan.n, plan.nz, plan.mats, plan.rows, plan.width
    L, R, half = plan.stages, plan.piece, plan.piece // 2
    (loaded, to_send, acc, row_old, col_old, row_part, row_mine, row_all, nr_sum, col_sum, w_sum, col_all, sq_all,
     load_sem, first_send, first_recv, old_sem, row_send, row_recv, col_send, col_recv, sq_send, sq_recv, *rest) = scratch
    recv, send_sem, recv_sem = rest[:L], rest[L:2 * L], rest[2 * L:3 * L]
    me, my_row = lax.axis_index("col"), lax.axis_index("row")
    peer = [flip(me, r) for r in range(n)]
    level = [lax.rem(my_row + i, nz) for i in range(nz)]
    first_half = lax.broadcasted_iota(jnp.int32, (1, LANES), 1) < LANES // 2
    far = [(i % nz, r) for i in range(1, nz + 1) for r in range(n - 1, -1, -1) if i < nz or r]

    def remote(src, dst, send, rcv, i, r):
        return pltpu.make_async_remote_copy(
            src_ref=src, dst_ref=dst, send_sem=send, recv_sem=rcv,
            device_id={"row": level[i], "col": peer[r]}, device_id_type=MESH,
        )

    def load(p, r):
        slot = lax.rem(p, plan.load_slots)
        at = pl.multiple_of(p * R, R)
        c = pl.multiple_of(peer[r] * width, LANES)
        group = int(r not in plan.first)
        j = plan.first.index(r ^ (group * plan.first_bit))
        return pltpu.make_async_copy(
            grad_terms.at[pl.ds(at, R), pl.ds(c, width)],
            loaded.at[slot, group, j],
            load_sem.at[slot, group],
        )

    def wait_load(p, group):
        slot = lax.rem(p, plan.load_slots)
        both = loaded.at[slot, group]
        pltpu.make_async_copy(both, both, load_sem.at[slot, group]).wait()

    def first_copy(p, r, h):
        a, b, j = lax.rem(p, plan.send_slots), lax.rem(p, plan.acc_slots), plan.first.index(r)
        at = pl.ds(h * half, half)
        return remote(
            to_send.at[a, j, at], acc.at[b, j, at], first_send.at[a], first_recv.at[lax.rem(p, 2), min(plan.units.index((r, h)), 2)],
            0, plan.first_bit,
        )

    def wait_first_sent(p):
        a = lax.rem(p, plan.send_slots)
        remote(to_send.at[a], to_send.at[a], first_send.at[a], first_recv.at[0, 0], 0, plan.first_bit).wait_send()

    def stage_copy(s, h, p, r):
        slot = lax.rem(p, plan.recv_slots[s - 1])
        bit = plan.orders[h][s]
        j = plan.kept[s - 1][h].index(r ^ bit)
        return remote(
            acc.at[lax.rem(p, plan.acc_slots), plan.first.index(r), pl.ds(h * half, half)],
            recv[s - 1].at[slot, h, j],
            send_sem[s - 1].at[lax.rem(p, plan.flight(s))],
            recv_sem[s - 1].at[slot],
            0,
            bit,
        )

    def wait_stage(s, p):
        slot = lax.rem(p, plan.recv_slots[s - 1])
        both = recv[s - 1].at[slot]
        remote(
            both, both, send_sem[s - 1].at[lax.rem(p, plan.flight(s))], recv_sem[s - 1].at[slot], 0, plan.orders[0][s]
        ).wait()

    def row_copy(k, r):
        at = lax.rem(k, plan.row_slots)
        return remote(row_all.at[k, me], row_all.at[k, me], row_send.at[at], row_recv.at[at], 0, r)

    def row_group(k):
        at, others = lax.rem(k, plan.row_slots), row_all.at[k, pl.ds(0, n - 1)]
        return remote(others, others, row_send.at[at], row_recv.at[at], 0, 1)

    def col_copy(m, i):
        return remote(col_all.at[m, my_row], col_all.at[m, my_row], col_send.at[m], col_recv.at[m], i, 0)

    def col_group(m):
        others = col_all.at[m, pl.ds(0, nz - 1)]
        return remote(others, others, col_send.at[m], col_recv.at[m], 1, 0)

    def sq_copy(m, i, r):
        here = sq_all.at[m, my_row * n + me]
        return remote(here, here, sq_send.at[m], sq_recv.at[m], i, r)

    def sq_group(m):
        others = sq_all.at[m, pl.ds(0, nz * n - 1)]
        return remote(others, others, sq_send.at[m], sq_recv.at[m], 1, 0)

    def load_step(p):
        for r in plan.first:
            load(p, r ^ plan.first_bit).start()
        for r in plan.first:
            load(p, r).start()

    def send_step(p):
        slot, into = lax.rem(p, plan.load_slots), lax.rem(p, plan.send_slots)
        pl.when(p >= plan.send_slots)(lambda: wait_first_sent(p - plan.send_slots))
        wait_load(p, 1)
        for r, h in plan.units:
            j = plan.first.index(r)

            @pl.loop(0, half // CHUNK)
            def _(i):
                at = pl.ds(pl.multiple_of(h * half + i * CHUNK, CHUNK), CHUNK)
                to_send[into, j, at] = loaded[slot, 1, j, at].astype(jnp.float32)

            first_copy(p, r, h).start()

    def stage_one(p):
        slot, a = lax.rem(p, plan.load_slots), lax.rem(p, plan.acc_slots)
        wait_load(p, 0)
        for r, h in plan.units:
            j = plan.first.index(r)
            if plan.units.index((r, h)) < 2:
                first_copy(p, r, h).wait_recv()
            elif plan.units.index((r, h)) == 2:
                rest = acc.at[a, pl.ds(0, n // 2 - 1)]
                remote(rest, rest, first_send.at[0], first_recv.at[lax.rem(p, 2), 2], 0, plan.first_bit).wait_recv()

            @pl.loop(0, half // CHUNK)
            def _(i):
                at = pl.ds(pl.multiple_of(h * half + i * CHUNK, CHUNK), CHUNK)
                acc[a, j, at] += loaded[slot, 0, j, at].astype(jnp.float32)

            if r in plan.sent[0][h]:
                stage_copy(1, h, p, r).start()

    def add_received(s, h, p):
        slot, a = lax.rem(p, plan.recv_slots[s - 1]), lax.rem(p, plan.acc_slots)
        for k, r in enumerate(plan.kept[s - 1][h]):
            j = plan.first.index(r)

            @pl.loop(0, half // CHUNK)
            def _(i):
                inside = pl.multiple_of(i * CHUNK, CHUNK)
                at = pl.ds(h * half + inside, CHUNK)
                acc[a, j, at] += recv[s - 1][slot, h, k, pl.ds(inside, CHUNK)]

    def stage_later(s, p):
        wait_stage(s - 1, p)
        for h in (0, 1):
            add_received(s - 1, h, p)
        for h in (0, 1):
            for r in plan.sent[s - 1][h]:
                stage_copy(s, h, p, r).start()

    def final_step(p):
        slot, a, m = lax.rem(p, plan.recv_slots[L - 1]), lax.rem(p, plan.acc_slots), (p * R) // rows
        own = plan.first.index(0)
        wait_stage(L, p)
        for h in (0, 1):

            @pl.loop(0, half // CHUNK)
            def _(i):
                inside = pl.multiple_of(i * CHUNK, CHUNK)
                at = h * half + inside
                g = acc[a, own, pl.ds(at, CHUNK)] + recv[L - 1][slot, h, 0, pl.ds(inside, CHUNK)]
                grad[pl.ds(p * R + at, CHUNK)] = g
                q = g * g + tiny_square
                lane = q[:, :LANES]
                for j in range(1, width // LANES):
                    lane = lane + q[:, j * LANES:(j + 1) * LANES]
                row_part[pl.ds(pl.multiple_of(lax.rem(p * R, LANES) + at, CHUNK), CHUNK)] = lane
                col_sum[m] += sum(q[8 * j:8 * j + 8] for j in range(CHUNK // 8))

        last = lax.rem((p + 1) * R, rows) == 0

        @pl.when(last)
        def _():
            col_all[m, my_row] = jnp.sum(col_sum[m], axis=0, keepdims=True)
            for i in range(nz - 1, 0, -1):
                col_copy(m, i).start()

        @pl.when(lax.rem((p + 1) * R, LANES) == 0)
        def _():
            k = (p * R) // LANES
            row_all[k, me] = jnp.sum(row_part[...].T, axis=0, keepdims=True)
            for r in range(n - 1, 0, -1):
                row_copy(k, r).start()

    def block_step(k):
        m = (k * LANES) // rows
        row_group(k).wait_recv()
        full = row_all[k, 0]
        for c in range(1, n):
            full = full + row_all[k, c]
        fresh = second_decay * row_mine[k] + (1.0 - second_decay) * full / ff
        row_mine[k] = fresh
        nr_sum[m] += fresh
        gain = jnp.broadcast_to(lax.rsqrt(fresh), (LANES, LANES)).T
        for i in range(LANES // 8):
            at = pl.ds(pl.multiple_of(k * LANES + 8 * i, 8), 8)
            by = gain[8 * i:8 * i + 8]
            for j in range(width // LANES):
                lanes = slice(j * LANES, (j + 1) * LANES)
                y = grad[at, lanes] * by
                grad[at, lanes] = y
                w_sum[m, :, lanes] += y * y
        row_group(k).wait_send()

    def matrix_step(m):
        col_group(m).wait_recv()
        full = col_all[m, 0]
        for z in range(1, nz):
            full = full + col_all[m, z]
        fresh = second_decay * col_old[pl.ds(m, 1), :] + (1.0 - second_decay) * full / d
        new_cols[pl.ds(m, 1), :] = fresh
        w = jnp.sum(w_sum[m], axis=0, keepdims=True) / fresh
        part = w[:, :LANES]
        for j in range(1, width // LANES):
            part = part + w[:, j * LANES:(j + 1) * LANES]
        both = [x + pltpu.roll(x, LANES // 2, 1) for x in (part, nr_sum[m])]
        sq_all[m, my_row * n + me] = jnp.where(first_half, *both)
        for i, r in far:
            sq_copy(m, i, r).start()
        col_group(m).wait_send()

    def scale_step(m):
        sq_group(m).wait_recv()
        both = jnp.sum(sq_all[m], axis=0)
        square = jnp.sum(jnp.where(first_half, both, 0.0), axis=1, keepdims=True)
        mean = jnp.sum(jnp.where(first_half, 0.0, both), axis=1, keepdims=True) / (n * d)
        clip = jnp.maximum(1.0, jnp.sqrt(square * mean / (d * ff)))
        col_gain[m:m + 1, :] = lax.rsqrt(new_cols[m:m + 1, :]) * (jnp.sqrt(mean) / clip)
        sq_group(m).wait_send()

    old_copies = [
        pltpu.make_async_copy(row_moment, row_old, old_sem.at[0]),
        pltpu.make_async_copy(col_moment, col_old, old_sem.at[1]),
    ]

    def old_step():
        for c in old_copies:
            c.wait()
        for m in range(mats):
            for k in range(rows // LANES):
                row_mine[m * (rows // LANES) + k] = row_old[m:m + 1, k * LANES:(k + 1) * LANES]

    o = plan.offset
    load_step(0)
    barrier = pltpu.get_barrier_semaphore()
    partners = [(i, 0) for i in range(nz - 1, 0, -1)] + [(0, bit) for bit in plan.orders[0]]
    for i, r in partners:
        pl.semaphore_signal(barrier, inc=1, device_id={"row": level[i], "col": peer[r]}, device_id_type=MESH)
    load_step(1)
    for c in old_copies:
        c.start()
    nr_sum[...] = jnp.zeros_like(nr_sum)
    col_sum[...] = jnp.zeros_like(col_sum)
    w_sum[...] = jnp.zeros_like(w_sum)
    pl.semaphore_wait(barrier, len(partners))

    per_block = LANES // R
    late = 2

    @pl.loop(-o[0], plan.pieces + 1)
    def _(t):
        def run(p, step):
            pl.when(jnp.logical_and(p >= 0, p < plan.pieces))(lambda: step(p))

        run(t + o[1], stage_one)
        for s in range(2, L + 1):
            run(t + o[s], functools.partial(stage_later, s))
        run(t - 1, final_step)
        run(t + o[0], send_step)
        pl.when(t + o[0] + 2 < plan.pieces)(lambda: load_step(t + o[0] + 2))
        pl.when(t == 0)(old_step)
        done = t - 1 - late

        @pl.when(jnp.logical_and(done >= 0, lax.rem(done + 1, per_block) == 0))
        def _():
            k = done // per_block
            block_step(k)
            pl.when(lax.rem((k + 1) * LANES, rows) == 0)(lambda: matrix_step((k * LANES) // rows))

    seen = plan.pieces - 1 - late
    for k in range((seen + 1) // per_block, plan.blocks):
        block_step(k)
        if (k + 1) * LANES % rows == 0:
            matrix_step(k * LANES // rows)
    for m in range(mats):
        for k in range(rows // LANES):
            new_rows[m:m + 1, k * LANES:(k + 1) * LANES] = row_mine[m * (rows // LANES) + k]
    for p in range(plan.pieces - plan.send_slots, plan.pieces):
        wait_first_sent(p)
    for m in range(mats):
        scale_step(m)


def finish(mats, grad, col_gain, rows_in, cols_in, update, new_rows, new_cols, scaled, small_sem, out_sem):
    total = grad.shape[0]
    small = [
        pltpu.make_async_copy(rows_in, new_rows, small_sem.at[0]),
        pltpu.make_async_copy(cols_in, new_cols, small_sem.at[1]),
    ]
    step = LANES // 2
    out = [
        pltpu.make_async_copy(scaled.at[pl.ds(c * step, step)], update.at[pl.ds(c * step, step)], out_sem)
        for c in range(total // step)
    ]
    for c in range(total // step):
        gain = jnp.broadcast_to(col_gain[c * step * mats // total:c * step * mats // total + 1, :], (8, grad.shape[1]))

        @pl.loop(0, step // 8, unroll=2)
        def _(i):
            at = pl.ds(pl.multiple_of(c * step + i * 8, 8), 8)
            scaled[at] = grad[at] * gain

        out[c].start()
        if c == 0:
            for s in small:
                s.start()
    for s in small:
        s.wait()
    pltpu.make_async_copy(scaled, update, out_sem).wait()


def on_device(n, nz, grad_terms, row_moment, col_moment):
    mats, rows, ff = grad_terms.shape[1:]
    width = ff // n
    d = rows * nz
    plan = Plan(n, nz, mats, rows, width)
    L, R, half, everyone = plan.stages, plan.piece, plan.piece // 2, n * nz
    kept = [len(plan.kept[s][0]) for s in range(L)]
    f32 = jnp.float32
    dma = pltpu.SemaphoreType.DMA
    blocks, total = plan.blocks, mats * rows
    scratch = [
        pltpu.VMEM((plan.load_slots, 2, n // 2, R, width), grad_terms.dtype),
        pltpu.VMEM((plan.send_slots, n // 2, R, width), f32),
        pltpu.VMEM((plan.acc_slots, n // 2, R, width), f32),
        pltpu.VMEM((mats, rows), f32),
        pltpu.VMEM((mats, width), f32),
        pltpu.VMEM((LANES, LANES), f32),
        pltpu.VMEM((blocks, 1, LANES), f32),
        pltpu.VMEM((blocks, n, 1, LANES), f32),
        pltpu.VMEM((mats, 1, LANES), f32),
        pltpu.VMEM((mats, 8, width), f32),
        pltpu.VMEM((mats, 8, width), f32),
        pltpu.VMEM((mats, nz, 1, width), f32),
        pltpu.VMEM((mats, everyone, 1, LANES), f32),
        dma((plan.load_slots, 2)),
        dma((plan.send_slots,)),
        dma((2, 3)),
        dma((2,)),
        dma((plan.row_slots,)),
        dma((plan.row_slots,)),
        dma((mats,)),
        dma((mats,)),
        dma((mats,)),
        dma((mats,)),
    ]
    scratch += [pltpu.VMEM((plan.recv_slots[s], 2, kept[s], half, width), f32) for s in range(L)]
    scratch += [dma((plan.flight(s + 1),)) for s in range(L)]
    scratch += [dma((plan.recv_slots[s],)) for s in range(L)]
    vmem, anywhere = pl.BlockSpec(memory_space=pltpu.VMEM), pl.BlockSpec(memory_space=pl.ANY)
    held = pl.pallas_call(
        functools.partial(kernel, plan, ff, d),
        out_shape=(
            pltpu.VMEM((total, width), f32),
            pltpu.VMEM((mats, width), f32),
            pltpu.VMEM((mats, rows), f32),
            pltpu.VMEM((mats, width), f32),
        ),
        in_specs=[anywhere] * 3,
        out_specs=(vmem,) * 4,
        scratch_shapes=scratch,
        compiler_params=pltpu.CompilerParams(
            collective_id=0, has_side_effects=True, vmem_limit_bytes=44 * 1024 * 1024
        ),
        name="reduce_and_level",
    )(grad_terms.reshape(total, ff), row_moment, col_moment)
    update, new_rows, new_cols = pl.pallas_call(
        functools.partial(finish, mats),
        out_shape=(
            jax.ShapeDtypeStruct((total, width), f32),
            jax.ShapeDtypeStruct((mats, rows), f32),
            jax.ShapeDtypeStruct((mats, width), f32),
        ),
        in_specs=[vmem] * 4,
        out_specs=(anywhere,) * 3,
        scratch_shapes=[pltpu.VMEM((total, width), f32), dma((2,)), dma],
        compiler_params=pltpu.CompilerParams(vmem_limit_bytes=24 * 1024 * 1024),
        name="scale_and_write",
    )(*held)
    return update.reshape(mats, rows, width), new_rows, new_cols


def solution(mesh):
    n, nz = mesh.shape["col"], mesh.shape["row"]
    return jax.shard_map(
        functools.partial(on_device, n, nz),
        mesh=mesh,
        in_specs=(P("col", None, "row", None), P(None, "row"), P(None, "col")),
        out_specs=(P(None, "row", "col"), P(None, "row"), P(None, "col")),
        check_vma=False,
    )
```

```python
import functools

import jax
import jax.numpy as jnp
from jax import lax
from jax.experimental import pallas as pl
from jax.experimental.pallas import tpu as pltpu
from jax.sharding import PartitionSpec as P

MESH = pl.DeviceIdType.MESH
second_decay = 1.0 - 100.0 ** (-0.8)
tiny_square = 1e-30
LANES = 128
PIECE = 64
CHUNK = 16


def flip(me, r):
    bit = 1
    while bit <= r:
        if r & bit:
            me = me + bit * (1 - 2 * lax.rem(me // bit, 2))
        bit *= 2
    return me


class Plan:
    def __init__(self, n, nz, mats, rows, width):
        bits = [1 << b for b in range(n.bit_length() - 1)]
        self.n, self.nz, self.mats, self.rows, self.width = n, nz, mats, rows, width
        self.orders = (bits, bits[:1] + bits[:0:-1])
        self.stages = len(bits) - 1
        self.first = [r for r in range(n) if not r & bits[0]]
        self.first_bit = bits[0]
        self.kept = []
        self.sent = []
        held = [list(self.first), list(self.first)]
        for s in range(1, self.stages + 1):
            sent = [[r for r in held[h] if r & self.orders[h][s]] for h in (0, 1)]
            held = [[r for r in held[h] if not r & self.orders[h][s]] for h in (0, 1)]
            self.sent.append(sent)
            self.kept.append([list(x) for x in held])
        early = [(r, h) for pair in zip(*(self.sent[0][h][::-1] for h in (0, 1))) for h, r in enumerate(pair)]
        late = [(r, h) for pair in zip(*(self.kept[0][h] for h in (0, 1))) for h, r in enumerate(pair)]
        self.units = early + late
        self.piece = PIECE
        self.pieces = mats * rows // self.piece
        self.blocks = mats * rows // LANES
        L = self.stages
        self.offset = [2 * (L - 1) + 1] + [2 * (L - s) for s in range(1, L + 1)]
        self.acc_slots = self.offset[0] + 5
        self.send_slots = 3
        self.load_slots = 3
        self.recv_slots = [6] * (L - 1) + [4]
        self.flight = lambda s: 3 if s < L else 2
        self.row_slots = -(-(self.offset[0] + 4) * self.piece // LANES)


def kernel(plan, ff, d, grad_terms, row_moment, col_moment, grad, col_gain, new_rows, new_cols, *scratch):
    n, nz, mats, rows, width = plan.n, plan.nz, plan.mats, plan.rows, plan.width
    L, R, half = plan.stages, plan.piece, plan.piece // 2
    (loaded, to_send, acc, row_old, col_old, row_part, row_mine, row_all, nr_sum, col_sum, w_sum, col_all, sq_all,
     load_sem, first_send, first_recv, old_sem, row_send, row_recv, col_send, col_recv, sq_send, sq_recv, *rest) = scratch
    recv, send_sem, recv_sem = rest[:L], rest[L:2 * L], rest[2 * L:3 * L]
    me, my_row = lax.axis_index("col"), lax.axis_index("row")
    peer = [flip(me, r) for r in range(n)]
    level = [lax.rem(my_row + i, nz) for i in range(nz)]
    first_half = lax.broadcasted_iota(jnp.int32, (1, LANES), 1) < LANES // 2
    far = [(i % nz, r) for i in range(1, nz + 1) for r in range(n - 1, -1, -1) if i < nz or r]

    def remote(src, dst, send, rcv, i, r):
        return pltpu.make_async_remote_copy(
            src_ref=src, dst_ref=dst, send_sem=send, recv_sem=rcv,
            device_id={"row": level[i], "col": peer[r]}, device_id_type=MESH,
        )

    def load(p, r):
        slot = lax.rem(p, plan.load_slots)
        at = pl.multiple_of(p * R, R)
        c = pl.multiple_of(peer[r] * width, LANES)
        group = int(r not in plan.first)
        j = plan.first.index(r ^ (group * plan.first_bit))
        return pltpu.make_async_copy(
            grad_terms.at[pl.ds(at, R), pl.ds(c, width)],
            loaded.at[slot, group, j],
            load_sem.at[slot, group],
        )

    def wait_load(p, group):
        slot = lax.rem(p, plan.load_slots)
        both = loaded.at[slot, group]
        pltpu.make_async_copy(both, both, load_sem.at[slot, group]).wait()

    def first_copy(p, r, h):
        a, b, j = lax.rem(p, plan.send_slots), lax.rem(p, plan.acc_slots), plan.first.index(r)
        at = pl.ds(h * half, half)
        return remote(
            to_send.at[a, j, at], acc.at[b, j, at], first_send.at[a], first_recv.at[lax.rem(p, 2), min(plan.units.index((r, h)), 2)],
            0, plan.first_bit,
        )

    def wait_first_sent(p):
        a = lax.rem(p, plan.send_slots)
        remote(to_send.at[a], to_send.at[a], first_send.at[a], first_recv.at[0, 0], 0, plan.first_bit).wait_send()

    def stage_copy(s, h, p, r):
        slot = lax.rem(p, plan.recv_slots[s - 1])
        bit = plan.orders[h][s]
        j = plan.kept[s - 1][h].index(r ^ bit)
        return remote(
            acc.at[lax.rem(p, plan.acc_slots), plan.first.index(r), pl.ds(h * half, half)],
            recv[s - 1].at[slot, h, j],
            send_sem[s - 1].at[lax.rem(p, plan.flight(s))],
            recv_sem[s - 1].at[slot],
            0,
            bit,
        )

    def wait_stage(s, p):
        slot = lax.rem(p, plan.recv_slots[s - 1])
        both = recv[s - 1].at[slot]
        remote(
            both, both, send_sem[s - 1].at[lax.rem(p, plan.flight(s))], recv_sem[s - 1].at[slot], 0, plan.orders[0][s]
        ).wait()

    def row_copy(k, r):
        at = lax.rem(k, plan.row_slots)
        return remote(row_all.at[k, me], row_all.at[k, me], row_send.at[at], row_recv.at[at], 0, r)

    def row_group(k):
        at, others = lax.rem(k, plan.row_slots), row_all.at[k, pl.ds(0, n - 1)]
        return remote(others, others, row_send.at[at], row_recv.at[at], 0, 1)

    def col_copy(m, i):
        return remote(col_all.at[m, my_row], col_all.at[m, my_row], col_send.at[m], col_recv.at[m], i, 0)

    def col_group(m):
        others = col_all.at[m, pl.ds(0, nz - 1)]
        return remote(others, others, col_send.at[m], col_recv.at[m], 1, 0)

    def sq_copy(m, i, r):
        here = sq_all.at[m, my_row * n + me]
        return remote(here, here, sq_send.at[m], sq_recv.at[m], i, r)

    def sq_group(m):
        others = sq_all.at[m, pl.ds(0, nz * n - 1)]
        return remote(others, others, sq_send.at[m], sq_recv.at[m], 1, 0)

    def load_step(p):
        for r in plan.first:
            load(p, r ^ plan.first_bit).start()
        for r in plan.first:
            load(p, r).start()

    def send_step(p):
        slot, into = lax.rem(p, plan.load_slots), lax.rem(p, plan.send_slots)
        pl.when(p >= plan.send_slots)(lambda: wait_first_sent(p - plan.send_slots))
        wait_load(p, 1)
        for r, h in plan.units:
            j = plan.first.index(r)

            @pl.loop(0, half // CHUNK)
            def _(i):
                at = pl.ds(pl.multiple_of(h * half + i * CHUNK, CHUNK), CHUNK)
                to_send[into, j, at] = loaded[slot, 1, j, at].astype(jnp.float32)

            first_copy(p, r, h).start()

    def stage_one(p):
        slot, a = lax.rem(p, plan.load_slots), lax.rem(p, plan.acc_slots)
        wait_load(p, 0)
        for r, h in plan.units:
            j = plan.first.index(r)
            if plan.units.index((r, h)) < 2:
                first_copy(p, r, h).wait_recv()
            elif plan.units.index((r, h)) == 2:
                rest = acc.at[a, pl.ds(0, n // 2 - 1)]
                remote(rest, rest, first_send.at[0], first_recv.at[lax.rem(p, 2), 2], 0, plan.first_bit).wait_recv()

            @pl.loop(0, half // CHUNK)
            def _(i):
                at = pl.ds(pl.multiple_of(h * half + i * CHUNK, CHUNK), CHUNK)
                acc[a, j, at] += loaded[slot, 0, j, at].astype(jnp.float32)

            if r in plan.sent[0][h]:
                stage_copy(1, h, p, r).start()

    def add_received(s, h, p):
        slot, a = lax.rem(p, plan.recv_slots[s - 1]), lax.rem(p, plan.acc_slots)
        for k, r in enumerate(plan.kept[s - 1][h]):
            j = plan.first.index(r)

            @pl.loop(0, half // CHUNK)
            def _(i):
                inside = pl.multiple_of(i * CHUNK, CHUNK)
                at = pl.ds(h * half + inside, CHUNK)
                acc[a, j, at] += recv[s - 1][slot, h, k, pl.ds(inside, CHUNK)]

    def stage_later(s, p):
        wait_stage(s - 1, p)
        for h in (0, 1):
            add_received(s - 1, h, p)
        for h in (0, 1):
            for r in plan.sent[s - 1][h]:
                stage_copy(s, h, p, r).start()

    def final_step(p):
        slot, a, m = lax.rem(p, plan.recv_slots[L - 1]), lax.rem(p, plan.acc_slots), (p * R) // rows
        own = plan.first.index(0)
        wait_stage(L, p)
        for h in (0, 1):

            @pl.loop(0, half // CHUNK)
            def _(i):
                inside = pl.multiple_of(i * CHUNK, CHUNK)
                at = h * half + inside
                g = acc[a, own, pl.ds(at, CHUNK)] + recv[L - 1][slot, h, 0, pl.ds(inside, CHUNK)]
                grad[pl.ds(p * R + at, CHUNK)] = g
                q = g * g + tiny_square
                lane = q[:, :LANES]
                for j in range(1, width // LANES):
                    lane = lane + q[:, j * LANES:(j + 1) * LANES]
                row_part[pl.ds(pl.multiple_of(lax.rem(p * R, LANES) + at, CHUNK), CHUNK)] = lane
                col_sum[m] += sum(q[8 * j:8 * j + 8] for j in range(CHUNK // 8))

        last = lax.rem((p + 1) * R, rows) == 0

        @pl.when(last)
        def _():
            col_all[m, my_row] = jnp.sum(col_sum[m], axis=0, keepdims=True)
            for i in range(nz - 1, 0, -1):
                col_copy(m, i).start()

        @pl.when(lax.rem((p + 1) * R, LANES) == 0)
        def _():
            k = (p * R) // LANES
            row_all[k, me] = jnp.sum(row_part[...].T, axis=0, keepdims=True)
            for r in range(n - 1, 0, -1):
                row_copy(k, r).start()

    def block_step(k):
        m = (k * LANES) // rows
        row_group(k).wait_recv()
        full = row_all[k, 0]
        for c in range(1, n):
            full = full + row_all[k, c]
        fresh = second_decay * row_mine[k] + (1.0 - second_decay) * full / ff
        row_mine[k] = fresh
        nr_sum[m] += fresh
        gain = jnp.broadcast_to(lax.rsqrt(fresh), (LANES, LANES)).T
        for i in range(LANES // 8):
            at = pl.ds(pl.multiple_of(k * LANES + 8 * i, 8), 8)
            by = gain[8 * i:8 * i + 8]
            for j in range(width // LANES):
                lanes = slice(j * LANES, (j + 1) * LANES)
                y = grad[at, lanes] * by
                grad[at, lanes] = y
                w_sum[m, :, lanes] += y * y
        row_group(k).wait_send()

    def matrix_step(m):
        col_group(m).wait_recv()
        full = col_all[m, 0]
        for z in range(1, nz):
            full = full + col_all[m, z]
        fresh = second_decay * col_old[pl.ds(m, 1), :] + (1.0 - second_decay) * full / d
        new_cols[pl.ds(m, 1), :] = fresh
        col_gain[pl.ds(m, 1), :] = lax.rsqrt(fresh)
        w = jnp.sum(w_sum[m], axis=0, keepdims=True) / fresh
        part = w[:, :LANES]
        for j in range(1, width // LANES):
            part = part + w[:, j * LANES:(j + 1) * LANES]
        both = [x + pltpu.roll(x, LANES // 2, 1) for x in (part, nr_sum[m])]
        sq_all[m, my_row * n + me] = jnp.where(first_half, *both)
        for i, r in far:
            sq_copy(m, i, r).start()
        col_group(m).wait_send()

    def scale_step(m):
        sq_group(m).wait_recv()
        both = jnp.sum(sq_all[m], axis=0)
        square = jnp.sum(jnp.where(first_half, both, 0.0), axis=1, keepdims=True)
        mean = jnp.sum(jnp.where(first_half, 0.0, both), axis=1, keepdims=True) / (n * d)
        clip = jnp.maximum(1.0, jnp.sqrt(square * mean / (d * ff)))
        col_gain[m:m + 1, :] = col_gain[m:m + 1, :] * (jnp.sqrt(mean) / clip)
        sq_group(m).wait_send()

    old_copies = [
        pltpu.make_async_copy(row_moment, row_old, old_sem.at[0]),
        pltpu.make_async_copy(col_moment, col_old, old_sem.at[1]),
    ]

    def old_step():
        for c in old_copies:
            c.wait()
        for m in range(mats):
            for k in range(rows // LANES):
                row_mine[m * (rows // LANES) + k] = row_old[m:m + 1, k * LANES:(k + 1) * LANES]

    o = plan.offset
    load_step(0)
    barrier = pltpu.get_barrier_semaphore()
    partners = [(i, 0) for i in range(nz - 1, 0, -1)] + [(0, bit) for bit in plan.orders[0]]
    for i, r in partners:
        pl.semaphore_signal(barrier, inc=1, device_id={"row": level[i], "col": peer[r]}, device_id_type=MESH)
    load_step(1)
    for c in old_copies:
        c.start()
    nr_sum[...] = jnp.zeros_like(nr_sum)
    col_sum[...] = jnp.zeros_like(col_sum)
    w_sum[...] = jnp.zeros_like(w_sum)
    pl.semaphore_wait(barrier, len(partners))

    per_block = LANES // R
    late = 2

    @pl.loop(-o[0], plan.pieces + 1)
    def _(t):
        def run(p, step):
            pl.when(jnp.logical_and(p >= 0, p < plan.pieces))(lambda: step(p))

        run(t + o[1], stage_one)
        run(t + o[0], send_step)
        for s in range(2, L + 1):
            run(t + o[s], functools.partial(stage_later, s))
        run(t - 1, final_step)
        pl.when(t + o[0] + 2 < plan.pieces)(lambda: load_step(t + o[0] + 2))
        pl.when(t == 0)(old_step)
        done = t - 1 - late

        @pl.when(jnp.logical_and(done >= 0, lax.rem(done + 1, per_block) == 0))
        def _():
            k = done // per_block
            block_step(k)
            pl.when(lax.rem((k + 1) * LANES, rows) == 0)(lambda: matrix_step((k * LANES) // rows))

    seen = plan.pieces - 1 - late
    for k in range((seen + 1) // per_block, plan.blocks):
        block_step(k)
        if (k + 1) * LANES % rows == 0:
            matrix_step(k * LANES // rows)
    for m in range(mats):
        for k in range(rows // LANES):
            new_rows[m:m + 1, k * LANES:(k + 1) * LANES] = row_mine[m * (rows // LANES) + k]
    for p in range(plan.pieces - plan.send_slots, plan.pieces):
        wait_first_sent(p)
    for m in range(mats):
        scale_step(m)


def finish(mats, grad, col_gain, rows_in, cols_in, update, new_rows, new_cols, scaled, small_sem, out_sem):
    total = grad.shape[0]
    small = [
        pltpu.make_async_copy(rows_in, new_rows, small_sem.at[0]),
        pltpu.make_async_copy(cols_in, new_cols, small_sem.at[1]),
    ]
    step = LANES // 2
    out = [
        pltpu.make_async_copy(scaled.at[pl.ds(c * step, step)], update.at[pl.ds(c * step, step)], out_sem)
        for c in range(total // step)
    ]
    for c in range(total // step):
        gain = jnp.broadcast_to(col_gain[c * step * mats // total:c * step * mats // total + 1, :], (8, grad.shape[1]))

        @pl.loop(0, step // 8, unroll=2)
        def _(i):
            at = pl.ds(pl.multiple_of(c * step + i * 8, 8), 8)
            scaled[at] = grad[at] * gain

        out[c].start()
        if c == 0:
            for s in small:
                s.start()
    for s in small:
        s.wait()
    pltpu.make_async_copy(scaled, update, out_sem).wait()


def on_device(n, nz, grad_terms, row_moment, col_moment):
    mats, rows, ff = grad_terms.shape[1:]
    width = ff // n
    d = rows * nz
    plan = Plan(n, nz, mats, rows, width)
    L, R, half, everyone = plan.stages, plan.piece, plan.piece // 2, n * nz
    kept = [len(plan.kept[s][0]) for s in range(L)]
    f32 = jnp.float32
    dma = pltpu.SemaphoreType.DMA
    blocks, total = plan.blocks, mats * rows
    scratch = [
        pltpu.VMEM((plan.load_slots, 2, n // 2, R, width), grad_terms.dtype),
        pltpu.VMEM((plan.send_slots, n // 2, R, width), f32),
        pltpu.VMEM((plan.acc_slots, n // 2, R, width), f32),
        pltpu.VMEM((mats, rows), f32),
        pltpu.VMEM((mats, width), f32),
        pltpu.VMEM((LANES, LANES), f32),
        pltpu.VMEM((blocks, 1, LANES), f32),
        pltpu.VMEM((blocks, n, 1, LANES), f32),
        pltpu.VMEM((mats, 1, LANES), f32),
        pltpu.VMEM((mats, 8, width), f32),
        pltpu.VMEM((mats, 8, width), f32),
        pltpu.VMEM((mats, nz, 1, width), f32),
        pltpu.VMEM((mats, everyone, 1, LANES), f32),
        dma((plan.load_slots, 2)),
        dma((plan.send_slots,)),
        dma((2, 3)),
        dma((2,)),
        dma((plan.row_slots,)),
        dma((plan.row_slots,)),
        dma((mats,)),
        dma((mats,)),
        dma((mats,)),
        dma((mats,)),
    ]
    scratch += [pltpu.VMEM((plan.recv_slots[s], 2, kept[s], half, width), f32) for s in range(L)]
    scratch += [dma((plan.flight(s + 1),)) for s in range(L)]
    scratch += [dma((plan.recv_slots[s],)) for s in range(L)]
    vmem, anywhere = pl.BlockSpec(memory_space=pltpu.VMEM), pl.BlockSpec(memory_space=pl.ANY)
    held = pl.pallas_call(
        functools.partial(kernel, plan, ff, d),
        out_shape=(
            pltpu.VMEM((total, width), f32),
            pltpu.VMEM((mats, width), f32),
            pltpu.VMEM((mats, rows), f32),
            pltpu.VMEM((mats, width), f32),
        ),
        in_specs=[anywhere] * 3,
        out_specs=(vmem,) * 4,
        scratch_shapes=scratch,
        compiler_params=pltpu.CompilerParams(
            collective_id=0, has_side_effects=True, vmem_limit_bytes=44 * 1024 * 1024
        ),
        name="reduce_and_level",
    )(grad_terms.reshape(total, ff), row_moment, col_moment)
    update, new_rows, new_cols = pl.pallas_call(
        functools.partial(finish, mats),
        out_shape=(
            jax.ShapeDtypeStruct((total, width), f32),
            jax.ShapeDtypeStruct((mats, rows), f32),
            jax.ShapeDtypeStruct((mats, width), f32),
        ),
        in_specs=[vmem] * 4,
        out_specs=(anywhere,) * 3,
        scratch_shapes=[pltpu.VMEM((total, width), f32), dma((2,)), dma],
        compiler_params=pltpu.CompilerParams(vmem_limit_bytes=24 * 1024 * 1024),
        name="scale_and_write",
    )(*held)
    return update.reshape(mats, rows, width), new_rows, new_cols


def solution(mesh):
    n, nz = mesh.shape["col"], mesh.shape["row"]
    return jax.shard_map(
        functools.partial(on_device, n, nz),
        mesh=mesh,
        in_specs=(P("col", None, "row", None), P(None, "row"), P(None, "col")),
        out_specs=(P(None, "row", "col"), P(None, "row"), P(None, "col")),
        check_vma=False,
    )
```
